256 devices in a mesh: gx: 8 (over y, core), gy: 32 (over z, x).
Axes of the slice: x: 4, y: 4, z: 8, core: 2. Of those that a mesh axis runs over, the one named last changes fastest.
Arguments:
- tokens: bfloat16 [1024, 4096], P('gy', 'gx'), may hold values from -140 to 140
- cotangent: bfloat16 [1024, 4096], P('gy', 'gx'), may hold values from -6 to 6
- gate_weight: bfloat16 [4096, 14336], P('gx', 'gy'), may hold values from -5 to 5
- up_weight: bfloat16 [4096, 14336], P('gx', 'gy'), may hold values from -5 to 5
- down_weight: bfloat16 [14336, 4096], P('gy', 'gx'), may hold values from -5 to 5
Outputs:
- output: bfloat16 [1024, 4096], P('gy', 'gx')
- input_grad: bfloat16 [1024, 4096], P('gy', 'gx')
- gate_grad: bfloat16 [4096, 14336], P('gx', 'gy')
- up_grad: bfloat16 [4096, 14336], P('gx', 'gy')
- down_grad: bfloat16 [14336, 4096], P('gy', 'gx')
The draws below stay inside these ranges and needn't reach their ends.
All inputs are finite; a program needn't handle non-finite values.
Results may differ from the reference program's by a relative error of at most 0.005.
The reference program's roundings to bfloat16 on the way count: a program that leaves them out, or rounds other values in their place, can miss the bound.
Values may be sent and summed in bfloat16 or wider, within the bound.
A program may use at most 64 MiB of HBM per device.

```python
import jax
import jax.numpy as jnp
from jax import lax

D = 4096
FF = 14336
ROT_BLOCK = 128
HID_BLOCK = 64
TOKENS = 1024


def rising_weight(key, row_total, col_total, fan_in):
    key_base, key_cols = jax.random.split(key)
    base = jnp.clip(jax.random.normal(key_base, (row_total, col_total), jnp.float32), -4.0, 4.0)
    row_frac = jnp.arange(row_total, dtype=jnp.float32)[:, None] / max(row_total - 1, 1)
    col_frac = jnp.arange(col_total, dtype=jnp.float32)[None, :] / max(col_total - 1, 1)
    col_rough = jnp.exp(jax.random.uniform(key_cols, (1, col_total), jnp.float32, 0.0, jnp.log(3.0)))
    rise = jnp.exp(jnp.log(3.0) * (row_frac + col_frac)) * col_rough
    return base * rise / (3.0 * fan_in ** 0.5)


def draw_tokens(key, part):
    key_base, key_rows, key_cols = jax.random.split(jax.random.fold_in(key, 11), 3)
    base = jnp.clip(jax.random.normal(key_base, (TOKENS, D), jnp.float32), -4.0, 4.0)
    row_rough = jnp.exp(jax.random.uniform(key_rows, (TOKENS, 1), jnp.float32, 0.0, jnp.log(3.3)))
    col_rough = jnp.exp(jax.random.uniform(key_cols, (1, D), jnp.float32, 0.0, jnp.log(3.0)))
    row_frac = jnp.arange(TOKENS, dtype=jnp.float32)[:, None] / max(TOKENS - 1, 1)
    col_frac = jnp.arange(D, dtype=jnp.float32)[None, :] / max(D - 1, 1)
    rise = jnp.exp(jnp.log(3.0) * (row_frac + col_frac))
    return (base * rise * row_rough * col_rough / 8.0).astype(jnp.bfloat16)


def draw_gate_weight(key, part):
    return rising_weight(jax.random.fold_in(key, 21), D, FF, D).astype(jnp.bfloat16)


def draw_up_weight(key, part):
    return rising_weight(jax.random.fold_in(key, 31), D, FF, D).astype(jnp.bfloat16)


def draw_down_weight(key, part):
    return rising_weight(jax.random.fold_in(key, 41), FF, D, FF).astype(jnp.bfloat16)


def block_levels(rng, extent, cuts, least, largest):
    loudness = 1.0
    for dim, parts in cuts:
        draws = jax.random.uniform(jax.random.fold_in(jax.random.fold_in(rng, 6), dim), (parts,), jnp.float32, least / len(cuts), largest / len(cuts))
        loudness = loudness * jnp.repeat(jnp.exp(draws), extent[dim] // parts).reshape((-1,) + (1,) * (len(extent) - 1 - dim))
    return loudness


def gaussian(own_key, shape, spread, most, cuts=(), kind=jnp.bfloat16):
    factor_of = block_levels(own_key, shape, cuts, -0.22, 0.18) if cuts else 1.0
    array = jax.random.normal(own_key, shape, jnp.float32) * spread * factor_of
    return jnp.minimum(jnp.maximum(array, -most), most).astype(kind)


def setup_inputs(seed: int = 0) -> dict:
    keys = jax.random.split(jax.random.key(seed), 6)
    return {
        "tokens": draw_tokens(jax.random.fold_in(keys[5], 71), 0),
        "cotangent": gaussian(keys[1], (TOKENS, D), 1.0, 6.0, ((0, 32), (1, 8))),
        "gate_weight": draw_gate_weight(jax.random.fold_in(keys[5], 71), 0),
        "up_weight": draw_up_weight(jax.random.fold_in(keys[5], 71), 0),
        "down_weight": draw_down_weight(jax.random.fold_in(keys[5], 71), 0),
    }


fp_top = 448.0
tiny = 1e-6


def hadamard_table(block_size):
    row_ids = jnp.arange(block_size, dtype=jnp.int32)[:, None]
    col_ids = jnp.arange(block_size, dtype=jnp.int32)[None, :]
    shared = row_ids & col_ids
    parity = jnp.zeros((block_size, block_size), jnp.int32)
    for bit_pos in range(max(block_size.bit_length() - 1, 1)):
        parity = parity + ((shared >> bit_pos) & 1)
    return (1 - 2 * (parity % 2)).astype(jnp.float32)


def rotate_cols(matrix, block_size):
    row_total, col_total = matrix.shape
    table = hadamard_table(block_size)
    blocks = matrix.astype(jnp.float32).reshape(row_total, col_total // block_size, block_size)
    turned = jnp.einsum("rbk,kl->rbl", blocks, table, precision=lax.Precision.HIGHEST)
    return turned.reshape(row_total, col_total) * (block_size ** -0.5)


def rotate_rows(matrix, block_size):
    row_total, col_total = matrix.shape
    table = hadamard_table(block_size)
    blocks = matrix.astype(jnp.float32).reshape(row_total // block_size, block_size, col_total)
    turned = jnp.einsum("kl,bkc->blc", table, blocks, precision=lax.Precision.HIGHEST)
    return turned.reshape(row_total, col_total) * (block_size ** -0.5)


def soft_cast(values, top):
    return (fp_top * jnp.tanh(values / (top + tiny))).astype(jnp.bfloat16)


def peak(values):
    return jnp.max(jnp.abs(values))


def reference(tokens, cotangent, gate_weight, up_weight, down_weight):
    token_rot = rotate_cols(tokens, ROT_BLOCK)
    gate_rot = rotate_rows(gate_weight, ROT_BLOCK)
    up_rot = rotate_rows(up_weight, ROT_BLOCK)
    down_rot = rotate_rows(down_weight, HID_BLOCK)
    token_peak = peak(token_rot)
    gate_peak = peak(gate_rot)
    up_peak = peak(up_rot)
    down_peak = peak(down_rot)
    token_cast = soft_cast(token_rot, token_peak)
    gate_cast = soft_cast(gate_rot, gate_peak)
    up_cast = soft_cast(up_rot, up_peak)
    down_cast = soft_cast(down_rot, down_peak)
    gate_pre = jnp.dot(token_cast, gate_cast, preferred_element_type=jnp.float32) * (token_peak * gate_peak / (fp_top * fp_top))
    up_pre = jnp.dot(token_cast, up_cast, preferred_element_type=jnp.float32) * (token_peak * up_peak / (fp_top * fp_top))
    hidden = (jax.nn.silu(gate_pre) * up_pre).astype(jnp.bfloat16)
    hidden_rot = rotate_cols(hidden, HID_BLOCK)
    hidden_peak = peak(hidden_rot)
    hidden_cast = soft_cast(hidden_rot, hidden_peak)
    output = (jnp.dot(hidden_cast, down_cast, preferred_element_type=jnp.float32) * (hidden_peak * down_peak / (fp_top * fp_top))).astype(jnp.bfloat16)
    down_grad = rotate_rows(jnp.dot(hidden_cast.T, cotangent, preferred_element_type=jnp.float32) * (hidden_peak / fp_top), HID_BLOCK).astype(jnp.bfloat16)
    hidden_grad = rotate_cols(jnp.dot(cotangent, down_cast.T, preferred_element_type=jnp.float32) * (down_peak / fp_top), HID_BLOCK)
    sigmoid_gate = jax.nn.sigmoid(gate_pre)
    gate_act = (hidden_grad * up_pre * sigmoid_gate * (1.0 + gate_pre * (1.0 - sigmoid_gate))).astype(jnp.bfloat16)
    up_act = (hidden_grad * gate_pre * sigmoid_gate).astype(jnp.bfloat16)
    gate_grad = rotate_rows(jnp.dot(token_cast.T, gate_act, preferred_element_type=jnp.float32) * (token_peak / fp_top), ROT_BLOCK).astype(jnp.bfloat16)
    up_grad = rotate_rows(jnp.dot(token_cast.T, up_act, preferred_element_type=jnp.float32) * (token_peak / fp_top), ROT_BLOCK).astype(jnp.bfloat16)
    input_sum = jnp.dot(gate_act, gate_cast.T, preferred_element_type=jnp.float32) * (gate_peak / fp_top) + jnp.dot(up_act, up_cast.T, preferred_element_type=jnp.float32) * (up_peak / fp_top)
    input_grad = rotate_cols(input_sum, ROT_BLOCK).astype(jnp.bfloat16)
    return (output, input_grad, gate_grad, up_grad, down_grad)
```

```python
import functools

import jax
import jax.numpy as jnp
from jax import lax
from jax.experimental import pallas as pl
from jax.experimental.pallas import tpu as pltpu
from jax.sharding import Mesh
from jax.sharding import PartitionSpec as P

GY = ("gy_0", "gy_1")
GX = ("gx_0", "gx_1")
NY, NC, NZ, NX = 4, 2, 8, 4
MESH = pl.DeviceIdType.MESH
f32 = jnp.float32
bf16 = jnp.bfloat16

TOP = 448.0
TINY = 1e-6
ROWS = 32
W = 512
HID = 448
PAIR = 2 * HID
R128 = 128 ** -0.5
R64 = 64 ** -0.5


def mm(a, b):
    return lax.dot_general(a, b, (((1,), (0,)), ((), ())), preferred_element_type=f32)


def mm_t(a, b):
    return lax.dot_general(a, b, (((1,), (1,)), ((), ())), preferred_element_type=f32)


def table(size, block):
    i = lax.broadcasted_iota(jnp.int32, (size, size), 0)
    j = lax.broadcasted_iota(jnp.int32, (size, size), 1)
    v = i & j & (block - 1)
    v = v ^ (v >> 4)
    v = v ^ (v >> 2)
    v = v ^ (v >> 1)
    sign = 1 - 2 * (v & 1)
    same = (i & ~(block - 1)) == (j & ~(block - 1))
    return jnp.where(same, sign, 0).astype(f32).astype(bf16)


def cut(n):
    at = 0
    while at < n:
        yield at, min(256, n - at)
        at += 256


def split(v, terms):
    parts = []
    for _ in range(terms):
        p = v.astype(bf16)
        parts.append(p)
        v = v - p.astype(f32)
    return parts


def turn_cols(v, h, terms=1):
    parts = split(v, terms) if terms > 1 else [v]
    outs = []
    for at, n in cut(v.shape[1]):
        outs.append(sum(mm(p[:, at : at + n], h[:n, :n]) for p in parts))
    return jnp.concatenate(outs, axis=1)


def encode(v, dst):
    hi = v.astype(bf16)
    dst[0:64] = hi
    hi = hi.astype(f32)
    unit = jnp.abs(hi) * (2.0**-8 / 7.0)
    n = jnp.where(unit > 0, (v - hi) / jnp.where(unit > 0, unit, 1.0), 0.0)
    n = jnp.clip(jnp.floor(n + 0.5), -7.0, 7.0) + 7.0
    dst[64:96] = (n[0:32] * 15.0 + n[32:64]).astype(bf16)


def decode(src):
    hi = src[0:64].astype(f32)
    code = src[64:96].astype(f32)
    first = jnp.floor((code + 0.5) * (1.0 / 15.0))
    n = jnp.concatenate([first, code - first * 15.0], axis=0) - 7.0
    return hi + n * (jnp.abs(hi) * (2.0**-8 / 7.0))


class Net:
    def __init__(self, send, recv):
        self.send_sems, self.recv_sems = send, recv
        self.n = 0
        self.all = []

    def send(self, src, dst, **dev):
        i = self.n
        self.n += 1
        names = {"y": "gx_0", "c": "gx_1", "z": "gy_0", "x": "gy_1"}
        d = pltpu.make_async_remote_copy(
            src_ref=src,
            dst_ref=dst,
            send_sem=self.send_sems.at[i],
            recv_sem=self.recv_sems.at[i],
            device_id={names[k]: v for k, v in dev.items()},
            device_id_type=MESH,
        )
        d.start()
        self.all.append(d)
        return d


class Peaks:
    def __init__(self, net, src, buf, me):
        self.net, self.src, self.buf = net, src, buf
        self.y, self.c, self.z, self.x = me

    def start(self, v):
        self.src[0] = v
        self.h = []
        for j in range(1, 8):
            dy, dc = j // 2, j % 2
            self.h.append(
                self.net.send(
                    self.src.at[0], self.buf.at[j - 1], y=(self.y + dy) % NY, c=(self.c + dc) % NC
                )
            )

    def gathered(self, level, at, n):
        for h in self.h:
            h.wait_recv()
        v = self.src[level]
        for j in range(n):
            v = jnp.maximum(v, self.buf[at + j])
        return v

    def second(self):
        self.src[1] = self.gathered(0, 0, 7)
        self.h = [
            self.net.send(self.src.at[1], self.buf.at[6 + j], x=(self.x + j) % NX)
            for j in range(1, NX)
        ]

    def third(self):
        self.src[2] = self.gathered(1, 7, 3)
        self.h = [
            self.net.send(self.src.at[2], self.buf.at[9 + j], z=(self.z + j) % NZ)
            for j in range(1, NZ)
        ]

    def result(self):
        return self.gathered(2, 10, 7)


N_SEMS = 220


def kernel(
    tok, cot, wg, wu, wd,
    out, ig, gg, ug, dg,
    h128, h64, t_all, c_all, tc, tct, rg, ru, rd, cg, cu, cd,
    pk_src, pk_buf, ph_src, ph_buf, pk, ph,
    dsrc, drecv, acc, ysrc, yrel, yfin, bsrc, brel, bfin,
    h_all, a_all, ch, cht, ga, ua,
    o_part, osrc, orel, ofin, ozs, ozr,
    i_part, isrc, irecv, ixs, ixr,
    ssem, rsem,
):
    y = lax.axis_index("gx_0")
    c = lax.axis_index("gx_1")
    z = lax.axis_index("gy_0")
    x = lax.axis_index("gy_1")
    pc = 1 - c
    net = Net(ssem, rsem)
    send = net.send
    yp, ym, y2 = (y + 1) % NY, (y + 3) % NY, (y + 2) % NY
    xp, xm, x2 = (x + 1) % NX, (x + 3) % NX, (x + 2) % NX
    zp, zm = (z + 1) % NZ, (z + 7) % NZ

    barrier = pltpu.get_barrier_semaphore()
    for j in range(1, 8):
        pl.semaphore_signal(
            barrier, inc=1, device_id={"gx_0": (y + j // 2) % NY, "gx_1": (c + j % 2) % NC},
            device_id_type=MESH,
        )
    for j in range(1, NX):
        pl.semaphore_signal(barrier, inc=1, device_id={"gy_1": (x + j) % NX}, device_id_type=MESH)
    for j in range(1, NZ):
        pl.semaphore_signal(barrier, inc=1, device_id={"gy_0": (z + j) % NZ}, device_id_type=MESH)
    h128[...] = table(256, 128)
    h64[...] = table(256, 64)
    t_all[z, x] = tok[...]
    c_all[z, x] = cot[...]
    pl.semaphore_wait(barrier, 7 + 3 + 7)

    def zat(d):
        return (z + d + NZ) % NZ

    xs = [(x + NX - j) % NX for j in range(NX)]
    tx, tzp, tzm = {}, {}, {}
    for j in range(1, NX):
        tx[j] = send(tok, t_all.at[z, x], x=(x + j) % NX)

    def t_step(s, j):
        if s < 3 or j < 2:
            b = zat(-s)
            src = tok if s == 0 and j == 0 else t_all.at[b, xs[j]]
            tzp[s, j] = send(src, t_all.at[b, xs[j]], z=zp)
        if s < 3 or j >= 2:
            b = zat(s)
            src = tok if s == 0 and j == 0 else t_all.at[b, xs[j]]
            tzm[s, j] = send(src, t_all.at[b, xs[j]], z=zm)

    def t_wait(s, j):
        if (s, j) in tzp:
            tzp[s, j].wait_recv()
        if (s, j) in tzm:
            tzm[s, j].wait_recv()

    czp, czm, cxp, cxm, crp, crm = {}, {}, {}, {}, {}, {}

    def c_step(s):
        if s < 3:
            bp, bm = zat(-s), zat(s)
            czp[s] = send(cot if s == 0 else c_all.at[bp, x], c_all.at[bp, x], z=zp)
            czm[s] = send(cot if s == 0 else c_all.at[bm, x], c_all.at[bm, x], z=zm)
        else:
            bp, bm = zat(-3), zat(3)
            lo = c_all.at[bp, x, pl.ds(0, 16)]
            hi = c_all.at[bm, x, pl.ds(16, 16)]
            czp[s] = send(lo, lo, z=zp)
            czm[s] = send(hi, hi, z=zm)

    def c_wait(s):
        czp[s].wait_recv()
        czm[s].wait_recv()

    def c_x(d):
        src = cot if d == 0 else c_all.at[zat(d), x]
        cxp[d] = send(src, c_all.at[zat(d), x], x=xp)
        cxm[d] = send(src, c_all.at[zat(d), x], x=xm)

    def c_relay(d):
        cxp[d].wait_recv()
        lo = c_all.at[zat(d), xm, pl.ds(0, 16)]
        crp[d] = send(lo, lo, x=xp)
        cxm[d].wait_recv()
        hi = c_all.at[zat(d), xp, pl.ds(16, 16)]
        crm[d] = send(hi, hi, x=xm)

    t_step(0, 0)
    c_step(0)
    c_x(0)

    p_x = jnp.max(jnp.abs(turn_cols(tok[...], h128))) * R128
    for at, n in cut(W):
        rg[at : at + n] = mm(h128[...], wg[at : at + n]) * R128
        ru[at : at + n] = mm(h128[...], wu[at : at + n]) * R128
    for at, n in cut(HID):
        rd[at : at + n] = mm(h64[:n, :n], wd[at : at + n]) * R64
    p_g = jnp.max(jnp.abs(rg[...]))
    p_u = jnp.max(jnp.abs(ru[...]))
    p_d = jnp.max(jnp.abs(rd[...]))
    row = lax.broadcasted_iota(jnp.int32, (8, 128), 0)
    peaks = Peaks(net, pk_src, pk_buf, (y, c, z, x))
    peaks.start(
        jnp.where(row == 0, p_x, jnp.where(row == 1, p_g, jnp.where(row == 2, p_u, p_d)))
    )
    for j in range(1, NX):
        tx[j].wait_recv()
        t_step(0, j)
    c_wait(0)
    c_step(1)
    c_x(1)
    c_x(-1)
    peaks.second()
    for j in range(NX):
        t_wait(0, j)
        t_step(1, j)
    c_wait(1)
    c_step(2)
    c_x(2)
    c_x(-2)
    c_relay(0)
    peaks.third()
    for j in range(NX):
        t_wait(1, j)
        t_step(2, j)
    c_wait(2)
    c_step(3)
    c_x(3)
    c_x(-3)
    c_relay(1)
    c_relay(-1)
    pk[...] = peaks.result()
    inv_x = 1.0 / (pk[0:1, 0:1] + TINY)
    cg[...] = (TOP * jnp.tanh(rg[...] * (1.0 / (pk[1:2, 0:1] + TINY)))).astype(bf16)
    cu[...] = (TOP * jnp.tanh(ru[...] * (1.0 / (pk[2:3, 0:1] + TINY)))).astype(bf16)
    cd[...] = (TOP * jnp.tanh(rd[...] * (1.0 / (pk[3:4, 0:1] + TINY)))).astype(bf16)
    for j in range(NX):
        t_wait(2, j)
        t_step(3, j)
    c_wait(3)
    c_x(4)
    c_relay(2)
    c_relay(-2)
    for j in range(NX):
        t_wait(3, j)
    c_relay(3)
    c_relay(-3)
    c_relay(4)

    def cast_tokens(k, carry):
        t = t_all[k].reshape(4 * ROWS, W)
        v = (TOP * jnp.tanh(turn_cols(t, h128) * R128 * inv_x)).astype(bf16)
        tc[k] = v
        tct[:, pl.ds(pl.multiple_of(k * 128, 128), 128)] = v.T
        return carry

    lax.fori_loop(0, 8, cast_tokens, 0)
    for d in (0, 1, -1, 2, -2, 3, -3, 4):
        crp[d].wait_recv()
        crm[d].wait_recv()

    def block(k, dst):
        t = tc[k]
        dst[0:128, 0:HID] = mm(t, cg[...]).astype(dst.dtype)
        dst[0:128, HID:PAIR] = mm(t, cu[...]).astype(dst.dtype)
        b = mm_t(c_all[k].reshape(4 * ROWS, W), cd[...]).astype(dst.dtype)
        dst[128:192, 0:HID] = b[0:64]
        dst[128:192, HID:PAIR] = b[64:128]

    order = [y2, yp, ym, y]
    dh = {}

    def both(i):
        block(order[i] * 2 + pc, dsrc.at[i])
        dh[i] = send(dsrc.at[i], drecv.at[i], c=pc)
        block(order[i] * 2 + c, acc.at[i])

    def q(i, at, n):
        return acc[i, at : at + n] + drecv[i, at : at + n]

    def put(slot, v, dst, **dev):
        encode(v, ysrc.at[slot])
        return send(ysrc.at[slot], dst, **dev)

    def put_h(slot, v, dst, **dev):
        bsrc[slot] = v.astype(bf16)
        return send(bsrc.at[slot], dst, **dev)

    both(0)
    both(1)
    dh[0].wait_recv()
    relp = put(0, q(0, 0, 64), yrel.at[0], y=yp)
    relm = put(1, q(0, 64, 64), yrel.at[1], y=ym)
    both(2)
    dh[1].wait_recv()
    fp_hi = put(2, q(1, 64, 64), yfin.at[0, 1], y=yp)
    dh[2].wait_recv()
    fm_lo = put(3, q(2, 0, 64), yfin.at[1, 0], y=ym)
    both(3)
    relp.wait_recv()
    fp_lo = put(4, q(1, 0, 64) + decode(yrel.at[0]), yfin.at[0, 0], y=yp)
    relm.wait_recv()
    fm_hi = put(5, q(2, 64, 64) + decode(yrel.at[1]), yfin.at[1, 1], y=ym)
    brp = put_h(0, q(0, 128, 32), brel.at[0], y=yp)
    brm = put_h(1, q(0, 160, 32), brel.at[1], y=ym)
    bp_hi = put_h(2, q(1, 160, 32), bfin.at[0, 1], y=yp)
    bm_lo = put_h(3, q(2, 128, 32), bfin.at[1, 0], y=ym)
    brp.wait_recv()
    bp_lo = put_h(4, q(1, 128, 32) + brel[0].astype(f32), bfin.at[0, 0], y=yp)
    brm.wait_recv()
    bm_hi = put_h(5, q(2, 160, 32) + brel[1].astype(f32), bfin.at[1, 1], y=ym)
    dh[3].wait_recv()
    for h in (fp_hi, fm_lo, fp_lo, fm_hi):
        h.wait_recv()
    for i in range(2):
        acc[3, 64 * i : 64 * i + 64] = (
            q(3, 64 * i, 64) + decode(yfin.at[0, i]) + decode(yfin.at[1, i])
        )

    p_x, p_g, p_u, p_d = (pk[i : i + 1, 0:1] for i in range(4))
    gate = acc[3, 0:128, 0:HID] * (p_x * p_g / (TOP * TOP))
    up = acc[3, 0:128, HID:PAIR] * (p_x * p_u / (TOP * TOP))
    s = jax.nn.sigmoid(gate)
    hid = (gate * s * up).astype(bf16)
    h_all[y, c, :, 0:HID] = hid[0:64]
    h_all[y, c, :, HID:PAIR] = hid[64:128]

    def gather(buf, half):
        own = buf.at[y, c]
        hs = {"own": send(own, own, c=pc)}
        hs["p"] = send(own, own, y=yp)
        hs["m"] = send(own, own, y=ym)
        return hs

    def gather_relay(buf, half, hs):
        hs["p"].wait_recv()
        lo = buf.at[ym, c, pl.ds(0, half)]
        hs["rp"] = send(lo, lo, y=yp)
        hs["m"].wait_recv()
        hi = buf.at[yp, c, pl.ds(half, half)]
        hs["rm"] = send(hi, hi, y=ym)
        hs["fp"] = send(buf.at[ym, c], buf.at[ym, c], c=pc)
        hs["fm"] = send(buf.at[yp, c], buf.at[yp, c], c=pc)

    def gather_last(buf, hs):
        hs["rp"].wait_recv()
        hs["rm"].wait_recv()
        hs["f2"] = send(buf.at[y2, c], buf.at[y2, c], c=pc)

    def gather_done(hs):
        for n in ("own", "fp", "fm", "f2"):
            hs[n].wait_recv()

    hh = gather(h_all, 32)
    hidp = Peaks(net, ph_src, ph_buf, (y, c, z, x))
    p_h = jnp.max(jnp.abs(turn_cols(hid, h64))) * R64
    hidp.start(jnp.full((8, 128), p_h, f32))

    for h in (bp_hi, bm_lo, bp_lo, bm_hi):
        h.wait_recv()
    b = q(3, 128, 64) + jnp.concatenate(
        [bfin[0, i].astype(f32) + bfin[1, i].astype(f32) for i in range(2)], axis=0
    )
    b = turn_cols(b * (p_d / TOP), h64, 3) * R64
    hg = jnp.concatenate([b[:, 0:HID], b[:, HID:PAIR]], axis=0)
    a_all[y, c, :, 0:HID] = (hg * up * s * (1.0 + gate * (1.0 - s))).astype(bf16)
    a_all[y, c, :, HID:PAIR] = (hg * gate * s).astype(bf16)
    ah = gather(a_all, 64)
    gather_relay(h_all, 32, hh)
    hidp.second()
    gather_last(h_all, hh)
    gather_relay(a_all, 64, ah)
    hidp.third()
    gather_done(hh)
    ph[...] = hidp.result()
    inv_h = 1.0 / (ph[0:1, 0:1] + TINY)

    def cast_hidden(k, carry):
        v = h_all[k // 2, k % 2]
        v = (TOP * jnp.tanh(turn_cols(v, h64) * R64 * inv_h)).astype(bf16)
        ch[k, 0:64] = v[:, 0:HID]
        ch[k, 64:128] = v[:, HID:PAIR]
        v = ch[k]
        cht[:, pl.ds(pl.multiple_of(k * 128, 128), 128)] = v.T
        o_part[k] = mm(v, cd[...]).reshape(NX, ROWS, W)
        return carry

    lax.fori_loop(0, 8, cast_hidden, 0)
    gather_last(a_all, ah)

    for d in range(NZ):
        osrc[0, d] = o_part[zat(d), x2].astype(bf16)
    L4, H4 = pl.ds(0, 4), pl.ds(4, 4)
    o_rp = send(osrc.at[0, L4], orel.at[0], x=xp)
    o_rm = send(osrc.at[0, H4], orel.at[1], x=xm)
    for d in range(4):
        osrc[1, 4 + d] = o_part[zat(4 + d), xp].astype(bf16)
        osrc[2, d] = o_part[zat(d), xm].astype(bf16)
    o_fph = send(osrc.at[1, H4], ofin.at[0, H4], x=xp)
    o_fml = send(osrc.at[2, L4], ofin.at[1, L4], x=xm)

    gather_done(ah)
    for k in range(8):
        ga[k] = a_all[k // 2, k % 2, :, 0:HID]
        ua[k] = a_all[k // 2, k % 2, :, HID:PAIR]

    def input_part(k):
        v = mm_t(ga[k], cg[...]) * (p_g / TOP) + mm_t(ua[k], cu[...]) * (p_u / TOP)
        i_part[k] = v.reshape(NX, ROWS, W)

    input_part(zat(4))
    isrc[0, 0] = i_part[zat(4)].astype(bf16)
    ip, im = {}, {}
    for j in range(NX):
        if j < 2:
            ip[0, j] = send(isrc.at[0, 0, j], irecv.at[0, 0, j], z=zp)
        else:
            im[0, j] = send(isrc.at[0, 0, j], irecv.at[1, 0, j], z=zm)

    o_rp.wait_recv()
    for d in range(4):
        osrc[1, d] = (o_part[zat(d), xp] + orel[0, d].astype(f32)).astype(bf16)
    o_fpl = send(osrc.at[1, L4], ofin.at[0, L4], x=xp)
    o_rm.wait_recv()
    for d in range(4):
        osrc[2, 4 + d] = (o_part[zat(4 + d), xm] + orel[1, d].astype(f32)).astype(bf16)
    o_fmh = send(osrc.at[2, H4], ofin.at[1, H4], x=xm)

    input_part(zat(3))
    input_part(zat(-3))

    def ring(s):
        for side, d, handles, dev in ((0, 4 - s, ip, zp), (1, s - 4, im, zm)):
            for j in (2, 3, 0, 1) if side == 0 else (0, 1, 2, 3):
                v = i_part[zat(d), j]
                if (s - 1, j) in handles:
                    handles[s - 1, j].wait_recv()
                    v = v + irecv[side, s - 1, j].astype(f32)
                isrc[side, s, j] = v.astype(bf16)
                handles[s, j] = send(isrc.at[side, s, j], irecv.at[side, s, j], z=dev)

    ring(1)
    input_part(zat(2))
    input_part(zat(-2))
    ring(2)
    input_part(zat(1))
    input_part(zat(-1))
    ring(3)
    input_part(z)

    for h in (o_fph, o_fml, o_fpl, o_fmh):
        h.wait_recv()
    oz = {}
    for d in range(NZ):
        v = o_part[zat(d), x] + ofin[0, d].astype(f32) + ofin[1, d].astype(f32)
        if d == 0:
            o_part[z, x] = v
        else:
            ozs[d] = v.astype(bf16)
            oz[d] = send(ozs.at[d], ozr.at[d], z=zat(d))

    for j in range(NX):
        ip[3, j].wait_recv()
        im[3, j].wait_recv()
        ixs[j] = (i_part[z, j] + irecv[0, 3, j].astype(f32) + irecv[1, 3, j].astype(f32)).astype(
            bf16
        )
    ix = {}
    for j in range(1, NX):
        ix[j] = send(ixs.at[(x + j) % NX], ixr.at[j], x=(x + j) % NX)

    p_h = ph[0:1, 0:1]

    def turn_rows(v, h, n):
        return sum(mm(h, p) for p in split(v, 2))

    for at, n in cut(HID):
        v = mm(cht[at : at + n], c_all[...].reshape(1024, W)) * (p_h / TOP)
        dg[at : at + n] = (turn_rows(v, h64[:n, :n], n) * R64).astype(bf16)
    for at, n in cut(W):
        for acts, dst in ((ga, gg), (ua, ug)):
            v = mm(tct[at : at + n], acts[...].reshape(1024, HID)) * (p_x / TOP)
            dst[at : at + n] = (turn_rows(v, h128[...], n) * R128).astype(bf16)

    v = o_part[z, x]
    for d in range(1, NZ):
        oz[d].wait_recv()
        v = v + ozr[d].astype(f32)
    out[...] = (v * (p_h * p_d / (TOP * TOP))).astype(bf16)

    v = i_part[z, x] + irecv[0, 3, x].astype(f32) + irecv[1, 3, x].astype(f32)
    for j in range(1, NX):
        ix[j].wait_recv()
        v = v + ixr[j].astype(f32)
    ig[...] = (turn_cols(v, h128, 3) * R128).astype(bf16)

    for h in net.all:
        h.wait_send()


def shards(tokens, cotangent, gate_weight, up_weight, down_weight):
    def vm(shape, dtype):
        return pltpu.VMEM(shape, dtype)

    scratch = [
        vm((256, 256), bf16), vm((256, 256), bf16),
        vm((NZ, NX, ROWS, W), bf16), vm((NZ, NX, ROWS, W), bf16),
        vm((8, 128, W), bf16), vm((W, 1024), bf16),
        vm((W, HID), f32), vm((W, HID), f32), vm((HID, W), f32),
        vm((W, HID), bf16), vm((W, HID), bf16), vm((HID, W), bf16),
        vm((3, 8, 128), f32), vm((17, 8, 128), f32), vm((3, 8, 128), f32), vm((17, 8, 128), f32),
        vm((8, 128), f32), vm((8, 128), f32),
        vm((4, 192, PAIR), f32), vm((4, 192, PAIR), f32), vm((4, 192, PAIR), f32),
        vm((6, 96, PAIR), bf16), vm((2, 96, PAIR), bf16), vm((2, 2, 96, PAIR), bf16),
        vm((6, 32, PAIR), bf16), vm((2, 32, PAIR), bf16), vm((2, 2, 32, PAIR), bf16),
        vm((NY, NC, 64, PAIR), bf16), vm((NY, NC, 128, PAIR), bf16),
        vm((8, 128, HID), bf16), vm((HID, 1024), bf16), vm((8, 128, HID), bf16), vm((8, 128, HID), bf16),
        vm((NZ, NX, ROWS, W), f32), vm((3, NZ, ROWS, W), bf16), vm((2, 4, ROWS, W), bf16),
        vm((2, NZ, ROWS, W), bf16), vm((NZ, ROWS, W), bf16), vm((NZ, ROWS, W), bf16),
        vm((NZ, NX, ROWS, W), f32), vm((2, 4, NX, ROWS, W), bf16), vm((2, 4, NX, ROWS, W), bf16),
        vm((NX, ROWS, W), bf16), vm((NX, ROWS, W), bf16),
        pltpu.SemaphoreType.DMA((N_SEMS,)), pltpu.SemaphoreType.DMA((N_SEMS,)),
    ]
    vmem = pl.BlockSpec(memory_space=pltpu.VMEM)
    return pl.pallas_call(
        kernel,
        out_shape=[
            jax.ShapeDtypeStruct((ROWS, W), bf16),
            jax.ShapeDtypeStruct((ROWS, W), bf16),
            jax.ShapeDtypeStruct((W, HID), bf16),
            jax.ShapeDtypeStruct((W, HID), bf16),
            jax.ShapeDtypeStruct((HID, W), bf16),
        ],
        in_specs=[vmem] * 5,
        out_specs=[vmem] * 5,
        scratch_shapes=scratch,
        compiler_params=pltpu.CompilerParams(
            collective_id=0, has_side_effects=True, vmem_limit_bytes=60 * 1024 * 1024
        ),
    )(tokens, cotangent, gate_weight, up_weight, down_weight)


def solution(mesh):
    fine = Mesh(mesh.devices.reshape(NY, NC, NZ, NX), GX + GY)
    specs = (P(GY, GX), P(GY, GX), P(GX, GY), P(GX, GY), P(GY, GX))
    return jax.shard_map(
        shards, mesh=fine, in_specs=specs, out_specs=specs, check_vma=False
    )
```

```python
import functools

import jax
import jax.numpy as jnp
from jax import lax
from jax.experimental import pallas as pl
from jax.experimental.pallas import tpu as pltpu
from jax.sharding import Mesh
from jax.sharding import PartitionSpec as P

GY = ("gy_0", "gy_1")
GX = ("gx_0", "gx_1")
NY, NC, NZ, NX = 4, 2, 8, 4
MESH = pl.DeviceIdType.MESH
f32 = jnp.float32
bf16 = jnp.bfloat16

TOP = 448.0
TINY = 1e-6
ROWS = 32
W = 512
HID = 448
PAIR = 2 * HID
R128 = 128 ** -0.5
R64 = 64 ** -0.5


def mm(a, b):
    return lax.dot_general(a, b, (((1,), (0,)), ((), ())), preferred_element_type=f32)


def mm_t(a, b):
    return lax.dot_general(a, b, (((1,), (1,)), ((), ())), preferred_element_type=f32)


def table(size, block):
    i = lax.broadcasted_iota(jnp.int32, (size, size), 0)
    j = lax.broadcasted_iota(jnp.int32, (size, size), 1)
    v = i & j & (block - 1)
    v = v ^ (v >> 4)
    v = v ^ (v >> 2)
    v = v ^ (v >> 1)
    sign = 1 - 2 * (v & 1)
    same = (i & ~(block - 1)) == (j & ~(block - 1))
    return jnp.where(same, sign, 0).astype(f32).astype(bf16)


def cut(n):
    at = 0
    while at < n:
        yield at, min(256, n - at)
        at += 256


def split(v, terms):
    parts = []
    for _ in range(terms):
        p = v.astype(bf16)
        parts.append(p)
        v = v - p.astype(f32)
    return parts


def turn_cols(v, h, terms=1):
    parts = split(v, terms) if terms > 1 else [v]
    outs = []
    for at, n in cut(v.shape[1]):
        outs.append(sum(mm(p[:, at : at + n], h[:n, :n]) for p in parts))
    return jnp.concatenate(outs, axis=1)


def encode(v, dst):
    hi = v.astype(bf16)
    dst[0:64] = hi
    hi = hi.astype(f32)
    unit = jnp.abs(hi) * (2.0**-8 / 7.0)
    n = jnp.where(unit > 0, (v - hi) / jnp.where(unit > 0, unit, 1.0), 0.0)
    n = jnp.clip(jnp.floor(n + 0.5), -7.0, 7.0) + 7.0
    dst[64:96] = (n[0:32] * 15.0 + n[32:64]).astype(bf16)


def decode(src):
    hi = src[0:64].astype(f32)
    code = src[64:96].astype(f32)
    first = jnp.floor((code + 0.5) * (1.0 / 15.0))
    n = jnp.concatenate([first, code - first * 15.0], axis=0) - 7.0
    return hi + n * (jnp.abs(hi) * (2.0**-8 / 7.0))


class Net:
    def __init__(self, send, recv):
        self.send_sems, self.recv_sems = send, recv
        self.n = self.phase = 0
        self.sent = [0] * N_PHASES

    def sem(self):
        self.n += 1
        return self.n - 1

    def copy(self, src, dst, sem, **dev):
        names = {"y": "gx_0", "c": "gx_1", "z": "gy_0", "x": "gy_1"}
        return pltpu.make_async_remote_copy(
            src_ref=src,
            dst_ref=dst,
            send_sem=self.send_sems.at[self.phase],
            recv_sem=self.recv_sems.at[sem],
            device_id={names[k]: v for k, v in dev.items()},
            device_id_type=MESH,
        )

    def count(self, src, copies=1):
        size = copies * src.dtype.itemsize
        for n in src.shape:
            size *= n
        self.sent[self.phase] += size

    def send(self, src, dst, sem=None, **dev):
        d = self.copy(src, dst, self.sem() if sem is None else sem, **dev)
        d.start()
        self.count(src)
        return d

    def wait(self, sem, ref):
        self.copy(ref, ref, sem, c=1 - lax.axis_index("gx_1")).wait_recv()

    def wait_sent(self, ref):
        for self.phase in range(N_PHASES):
            part = ref.at[pl.ds(0, self.sent[self.phase] // 4096)]
            self.copy(part, part, 0, c=1 - lax.axis_index("gx_1")).wait_send()


class Peaks:
    def __init__(self, net, src, buf, me):
        self.net, self.src, self.buf = net, src, buf
        self.y, self.c, self.z, self.x = me

    def start(self, v):
        self.src[0] = v
        self.sem = self.net.sem()
        for j in range(1, 8):
            dy, dc = j // 2, j % 2
            self.net.send(
                self.src.at[0], self.buf.at[j - 1], self.sem, y=(self.y + dy) % NY, c=(self.c + dc) % NC
            )

    def gathered(self, level, at, n):
        self.net.wait(self.sem, self.buf.at[pl.ds(at, n)])
        v = self.src[level]
        for j in range(n):
            v = jnp.maximum(v, self.buf[at + j])
        return v

    def second(self):
        self.src[1] = self.gathered(0, 0, 7)
        self.sem = self.net.sem()
        for j in range(1, NX):
            self.net.send(self.src.at[1], self.buf.at[6 + j], self.sem, x=(self.x + j) % NX)

    def third(self):
        self.src[2] = self.gathered(1, 7, 3)
        self.sem = self.net.sem()
        for j in range(1, NZ):
            self.net.send(self.src.at[2], self.buf.at[9 + j], self.sem, z=(self.z + j) % NZ)

    def result(self):
        return self.gathered(2, 10, 7)


class ZX:
    def __init__(self, net, own, buf, z, x):
        self.net, self.own, self.buf, self.z, self.x = net, own, buf, z, x
        self.came, self.crossed = {}, {}
        self.relays = net.sem()

    def at(self, d):
        return (self.z + d + NZ) % NZ

    def start(self):
        for d in (1, -1, 2, -2, 3, -3, 4):
            h = self.net.send(self.own, self.buf.at[self.z, self.x], z=self.at(d))
            self.came[4 if d == 4 else -d] = h

    def cross(self, d):
        b = self.at(d)
        src = self.own
        if d:
            self.came[d].wait_recv()
            src = self.buf.at[b, self.x]
        self.crossed[d] = self.net.sem()
        for k in (1, 3):
            self.net.send(src, self.buf.at[b, self.x], self.crossed[d], x=(self.x + k) % NX)

    def relay(self, d):
        b, xp, xm = self.at(d), (self.x + 1) % NX, (self.x + 3) % NX
        self.net.wait(self.crossed[d], self.buf.at[0, pl.ds(0, 2)])
        lo = self.buf.at[b, xm, pl.ds(0, 16)]
        self.net.send(lo, lo, self.relays, x=xp)
        hi = self.buf.at[b, xp, pl.ds(16, 16)]
        self.net.send(hi, hi, self.relays, x=xm)

    def done(self):
        self.net.wait(self.relays, self.buf.at[pl.ds(0, 2)])


class Gather:
    def __init__(self, net, buf, half, y, c, together):
        self.net, self.buf, self.half, self.y, self.c = net, buf, half, y, c
        self.yp, self.ym, self.y2 = (y + 1) % NY, (y + 3) % NY, (y + 2) % NY
        self.pair = net.sem() if together else None
        self.rest = net.sem()

    def part(self, y, i):
        return self.buf.at[y, self.c, pl.ds(i * self.half, self.half)]

    def to_pair(self, y):
        return self.net.send(self.buf.at[y, self.c], self.buf.at[y, self.c], self.pair, c=1 - self.c)

    def start(self):
        send, y = self.net.send, self.y
        self.p0 = send(self.part(y, 0), self.part(y, 0), y=self.yp)
        self.m1 = send(self.part(y, 1), self.part(y, 1), y=self.ym)
        self.p1 = send(self.part(y, 1), self.part(y, 1), y=self.yp)
        self.m0 = send(self.part(y, 0), self.part(y, 0), y=self.ym)
        self.own = self.to_pair(y)

    def relay(self):
        send = self.net.send
        self.p0.wait_recv()
        send(self.part(self.ym, 0), self.part(self.ym, 0), self.rest, y=self.yp)
        self.m1.wait_recv()
        send(self.part(self.yp, 1), self.part(self.yp, 1), self.rest, y=self.ym)

    def share(self):
        self.p1.wait_recv()
        self.fp = self.to_pair(self.ym)
        self.m0.wait_recv()
        self.fm = self.to_pair(self.yp)

    def last(self):
        self.net.wait(self.rest, self.buf.at[0, 0])
        self.f2 = self.to_pair(self.y2)

    def done(self):
        self.net.wait(self.pair, self.buf.at[:, 0])


N_SEMS = 110
N_PHASES = 5
MOST_SENT = 1280
RELATIVE = (4, 3, -3, 2, -2, 1, -1, 0)


def kernel(
    tok, cot, wg_hbm, wu_hbm, wd_hbm,
    gg_hbm, ug_hbm, dg_hbm, out_hbm, ig_hbm,
    h128, h64, wts, t_all, c_all, tc, rg, ru, rd, cg, cu, cd,
    pk_src, pk_buf, ph_src, ph_buf, pk, ph,
    dsrc, drecv, acc, ysrc, yrel, yfin, esrc, erecv, eacc, bsrc, brel, bfin,
    h_all, a_all, hrot, cht, gat, uat,
    o_part, osrc, orecv, oxs, oxr,
    i_part, isrc, irel, ifin, izf, izs, izr,
    small, grads, unread,
    ssem, rsem, lsem,
):
    y = lax.axis_index("gx_0")
    c = lax.axis_index("gx_1")
    z = lax.axis_index("gy_0")
    x = lax.axis_index("gy_1")
    pc = 1 - c
    net = Net(ssem, rsem)
    send = net.send
    yp, ym, y2 = (y + 1) % NY, (y + 3) % NY, (y + 2) % NY
    xp, xm, x2 = (x + 1) % NX, (x + 3) % NX, (x + 2) % NX
    zp, zm = (z + 1) % NZ, (z + 7) % NZ

    def zat(d):
        return (z + d + NZ) % NZ

    barrier = pltpu.get_barrier_semaphore()
    for j in range(1, 8):
        pl.semaphore_signal(
            barrier, inc=1, device_id={"gx_0": (y + j // 2) % NY, "gx_1": (c + j % 2) % NC},
            device_id_type=MESH,
        )
    for j in range(1, NX):
        pl.semaphore_signal(barrier, inc=1, device_id={"gy_1": (x + j) % NX}, device_id_type=MESH)
    for j in range(1, NZ):
        pl.semaphore_signal(barrier, inc=1, device_id={"gy_0": (z + j) % NZ}, device_id_type=MESH)
    loads = [
        pltpu.make_async_copy(w, wts.at[i], lsem.at[i]) for i, w in enumerate((wg_hbm, wu_hbm, wd_hbm))
    ]
    for load in loads:
        load.start()
    h128[...] = table(256, 128)
    h64[...] = table(256, 64)
    t_all[z, x] = tok[...]
    c_all[z, x] = cot[...]
    for load in loads:
        load.wait()

    def rotate_weights():
        rg[...] = turn_cols(wts[0], h128) * R128
        ru[...] = turn_cols(wts[1], h128) * R128
        for at, n in cut(HID):
            rd[at : at + n] = mm(h64[:n, :n], wts[2, at : at + n]) * R64

    p_x = jnp.max(jnp.abs(turn_cols(tok[...], h128))) * R128
    rotate_weights()
    p_g = jnp.max(jnp.abs(rg[...]))
    p_u = jnp.max(jnp.abs(ru[...]))
    p_d = jnp.max(jnp.abs(rd[...]))
    row = lax.broadcasted_iota(jnp.int32, (8, 128), 0)
    own_peaks = jnp.where(row == 0, p_x, jnp.where(row == 1, p_g, jnp.where(row == 2, p_u, p_d)))
    pl.semaphore_wait(barrier, 7 + 3 + 7)

    T = ZX(net, tok, t_all, z, x)
    C = ZX(net, cot, c_all, z, x)
    peaks = Peaks(net, pk_src, pk_buf, (y, c, z, x))
    T.start()
    peaks.start(own_peaks)
    T.cross(0)
    T.cross(1)
    T.cross(-1)
    T.relay(0)
    peaks.second()
    T.cross(2)
    T.cross(-2)
    T.relay(1)
    T.relay(-1)
    peaks.third()
    net.phase = 1
    C.start()
    T.cross(3)
    T.cross(-3)
    T.relay(2)
    T.relay(-2)
    T.cross(4)
    T.relay(3)
    T.relay(-3)
    C.cross(0)
    pk[...] = peaks.result()
    inv_x = 1.0 / (pk[0:1, 0:1] + TINY)
    cg[...] = (TOP * jnp.tanh(rg[...] * (1.0 / (pk[1:2, 0:1] + TINY)))).astype(bf16)
    cu[...] = (TOP * jnp.tanh(ru[...] * (1.0 / (pk[2:3, 0:1] + TINY)))).astype(bf16)
    T.relay(4)
    T.done()
    C.cross(1)
    C.cross(-1)
    C.relay(0)

    def gate_up(k, dst):
        t = turn_cols(t_all[k].reshape(4 * ROWS, W), h128)
        t = (TOP * jnp.tanh(t * (R128 * inv_x))).astype(bf16)
        tc[k] = t
        dst[:, 0:HID] = mm_t(t, cg[...])
        dst[:, HID:PAIR] = mm_t(t, cu[...])

    order = [y2, yp, ym, y]
    dh, eh = {}, {}

    def both(i):
        gate_up(order[i] * 2 + pc, dsrc.at[i])
        dh[i] = send(dsrc.at[i], drecv.at[i], c=pc)
        gate_up(order[i] * 2 + c, acc.at[i])

    def q(i, at):
        return acc[i, at : at + 64] + drecv[i, at : at + 64]

    def put(slot, v, dst, sem=None, **dev):
        encode(v, ysrc.at[slot])
        return send(ysrc.at[slot], dst, sem, **dev)

    net.phase = 2
    y_fin, b_fin = net.sem(), net.sem()
    both(0)
    both(1)
    dh[0].wait_recv()
    relp = put(0, q(0, 0), yrel.at[0], y=yp)
    relm = put(1, q(0, 64), yrel.at[1], y=ym)
    both(2)
    dh[1].wait_recv()
    put(2, q(1, 64), yfin.at[0, 1], y_fin, y=yp)
    dh[2].wait_recv()
    put(3, q(2, 0), yfin.at[1, 0], y_fin, y=ym)
    C.cross(2)
    C.cross(-2)
    C.relay(1)
    C.relay(-1)
    cd[...] = (TOP * jnp.tanh(rd[...] * (1.0 / (pk[3:4, 0:1] + TINY)))).astype(bf16)
    C.cross(3)
    C.cross(-3)
    C.relay(2)
    C.relay(-2)
    C.cross(4)
    relp.wait_recv()
    put(4, q(1, 0) + decode(yrel.at[0]), yfin.at[0, 0], y_fin, y=yp)
    relm.wait_recv()
    put(5, q(2, 64) + decode(yrel.at[1]), yfin.at[1, 1], y_fin, y=ym)
    both(3)
    C.relay(3)
    C.relay(-3)
    C.relay(4)
    C.done()

    def back(k, dst):
        b = mm_t(c_all[k].reshape(4 * ROWS, W), cd[...])
        dst[:, 0:HID] = b[0:64]
        dst[:, HID:PAIR] = b[64:128]

    def both_back(i):
        back(order[i] * 2 + pc, esrc.at[i])
        eh[i] = send(esrc.at[i], erecv.at[i], c=pc)
        back(order[i] * 2 + c, eacc.at[i])

    def e(i, at):
        return eacc[i, at : at + 32] + erecv[i, at : at + 32]

    def put_b(slot, v, dst, sem=None, **dev):
        bsrc[slot] = v.astype(bf16)
        return send(bsrc.at[slot], dst, sem, **dev)

    both_back(0)
    both_back(1)
    eh[0].wait_recv()
    brp = put_b(0, e(0, 0), brel.at[0], y=yp)
    brm = put_b(1, e(0, 32), brel.at[1], y=ym)
    both_back(2)
    eh[1].wait_recv()
    put_b(2, e(1, 32), bfin.at[0, 1], b_fin, y=yp)
    eh[2].wait_recv()
    put_b(3, e(2, 0), bfin.at[1, 0], b_fin, y=ym)
    both_back(3)

    dh[3].wait_recv()
    net.wait(y_fin, yfin)
    for i in range(2):
        acc[3, 64 * i : 64 * i + 64] = q(3, 64 * i) + decode(yfin.at[0, i]) + decode(yfin.at[1, i])
    p_x, p_g, p_u, p_d = (pk[i : i + 1, 0:1] for i in range(4))
    gate = acc[3, :, 0:HID] * (p_x * p_g / (TOP * TOP))
    up = acc[3, :, HID:PAIR] * (p_x * p_u / (TOP * TOP))
    s = jax.nn.sigmoid(gate)
    hid = (gate * s * up).astype(bf16)
    h_all[y, c, :, 0:HID] = hid[0:64]
    h_all[y, c, :, HID:PAIR] = hid[64:128]
    hidp = Peaks(net, ph_src, ph_buf, (y, c, z, x))
    p_h = jnp.max(jnp.abs(turn_cols(hid, h64))) * R64
    hidp.start(jnp.full((8, 128), p_h, f32))
    net.phase = 3
    H = Gather(net, h_all, 32, y, c, True)
    H.start()
    brp.wait_recv()
    put_b(4, e(1, 0) + brel[0].astype(f32), bfin.at[0, 0], b_fin, y=yp)
    brm.wait_recv()
    put_b(5, e(2, 32) + brel[1].astype(f32), bfin.at[1, 1], b_fin, y=ym)
    hidp.second()
    H.relay()
    eh[3].wait_recv()
    net.wait(b_fin, bfin)
    b = jnp.concatenate(
        [e(3, 32 * i) + bfin[0, i].astype(f32) + bfin[1, i].astype(f32) for i in range(2)], axis=0
    )
    b = turn_cols(b * (p_d / TOP), h64, 3) * R64
    hg = jnp.concatenate([b[:, 0:HID], b[:, HID:PAIR]], axis=0)
    a_all[y, c, :, 0:HID] = (hg * up * s * (1.0 + gate * (1.0 - s))).astype(bf16)
    a_all[y, c, :, HID:PAIR] = (hg * gate * s).astype(bf16)
    G = Gather(net, a_all, 64, y, c, False)
    G.start()
    hidp.third()
    H.share()
    H.last()
    H.done()

    def turn_hidden(k, carry):
        hrot[k] = turn_cols(h_all[k // 2, k % 2], h64) * R64
        return carry

    lax.fori_loop(0, 8, turn_hidden, 0)
    ph[...] = hidp.result()
    p_h = ph[0:1, 0:1]
    inv_h = 1.0 / (p_h + TINY)

    def o_block(d):
        k = zat(d)
        v = (TOP * jnp.tanh(hrot[k] * inv_h)).astype(bf16)
        v = jnp.concatenate([v[:, 0:HID], v[:, HID:PAIR]], axis=0)
        cht[:, pl.ds(pl.multiple_of(k * 128, 128), 128)] = v.T
        o_part[RELATIVE.index(d)] = mm(v, cd[...]).reshape(NX, ROWS, W)

    op, om = {}, {}
    o_last, o_cross = net.sem(), net.sem()

    def o_ring(s):
        for side, d, handles, dev in ((0, 4 - s, op, zp), (1, s - 4, om, zm)):
            i = RELATIVE.index(4 if s == 0 else d)
            for j in (2, 3, 0, 1) if side == 0 else (0, 1, 2, 3):
                if s == 0 and (j < 2) != (side == 0):
                    continue
                v = o_part[i, j]
                if (s - 1, j) in handles:
                    handles[s - 1, j].wait_recv()
                    v = v + orecv[side, s - 1, j].astype(f32)
                osrc[side, s, j] = v.astype(bf16)
                sem = o_last if s == 3 else None
                handles[s, j] = send(osrc.at[side, s, j], orecv.at[side, s, j], sem, z=dev)

    blocks = [(y, c), (y, pc), (ym, c), (yp, c), (ym, pc), (yp, pc), (y2, c), (y2, pc)]
    ir = {}
    i_fin = [net.sem() for _ in range(8)]
    i_owner = net.sem()

    def i_block(n):
        yy, cc = blocks[n]
        g = a_all[yy, cc, :, 0:HID]
        u = a_all[yy, cc, :, HID:PAIR]
        v = mm(g, cg[...]) * (p_g / TOP) + mm(u, cu[...]) * (p_u / TOP)
        i_part[n] = v.reshape(NX, ROWS, W)
        isrc[n, 0] = i_part[n, x2].astype(bf16)
        if n % 2 == 0:
            ir[n] = send(isrc.at[n, 0], irel.at[n], x=xp)
            isrc[n, 2] = i_part[n, xm].astype(bf16)
            send(isrc.at[n, 2], ifin.at[n, 1], i_fin[n], x=xm)
        else:
            ir[n] = send(isrc.at[n, 0], irel.at[n], x=xm)
            isrc[n, 1] = i_part[n, xp].astype(bf16)
            send(isrc.at[n, 1], ifin.at[n, 0], i_fin[n], x=xp)
        lanes = pl.ds(pl.multiple_of((yy * 2 + cc) * 128, 128), 128)
        gat[:, lanes] = g.T
        uat[:, lanes] = u.T

    def i_relay(n):
        ir[n].wait_recv()
        if n % 2 == 0:
            isrc[n, 1] = (i_part[n, xp] + irel[n].astype(f32)).astype(bf16)
            send(isrc.at[n, 1], ifin.at[n, 0], i_fin[n], x=xp)
        else:
            isrc[n, 2] = (i_part[n, xm] + irel[n].astype(f32)).astype(bf16)
            send(isrc.at[n, 2], ifin.at[n, 1], i_fin[n], x=xm)

    def i_final(n):
        yy, cc = blocks[n]
        net.wait(i_fin[n], ifin.at[n])
        k = yy * 2 + cc
        d = (k + NZ - z) % NZ
        v = i_part[n, x] + ifin[n, 0].astype(f32) + ifin[n, 1].astype(f32)
        izf[d] = v
        izs[d] = v.astype(bf16)

        @pl.when(d != 0)
        def _():
            net.copy(izs.at[d], izr.at[d], i_owner, z=k).start()

    net.phase = 4
    o_block(4)
    o_ring(0)
    G.relay()
    i_block(0)
    G.own.wait_recv()
    i_block(1)
    G.share()
    o_block(3)
    o_block(-3)
    o_ring(1)
    i_block(2)
    i_block(3)
    i_relay(0)
    i_relay(1)
    o_block(2)
    o_block(-2)
    G.last()
    o_ring(2)
    i_final(0)
    i_final(1)
    G.fp.wait_recv()
    i_block(4)
    G.fm.wait_recv()
    i_block(5)
    i_relay(2)
    i_relay(3)
    o_block(1)
    o_block(-1)
    i_block(6)
    G.f2.wait_recv()
    i_block(7)
    o_ring(3)
    i_final(2)
    i_final(3)
    i_relay(4)
    i_relay(5)
    o_block(0)
    i_relay(6)
    i_relay(7)
    i_final(4)
    i_final(5)

    stores = []

    def store(src, dst):
        copy = pltpu.make_async_copy(src, dst, lsem.at[3 + len(stores)])
        copy.start()
        stores.append(copy)

    for at, n in cut(HID):
        v = mm(cht[at : at + n], c_all[...].reshape(1024, W)) * (p_h / TOP)
        grads[2, at : at + n] = (sum(mm(h64[:n, :n], p) for p in split(v, 2)) * R64).astype(bf16)
    store(grads.at[2], dg_hbm)
    net.wait(o_last, orecv.at[:, 3])
    for j in range(NX):
        o_part[7, j] = o_part[7, j] + orecv[0, 3, j].astype(f32) + orecv[1, 3, j].astype(f32)
        oxs[j] = o_part[7, j].astype(bf16)
    for j in range(1, NX):
        send(oxs.at[(x + j) % NX], oxr.at[j], o_cross, x=(x + j) % NX)
    i_final(6)
    i_final(7)
    for i, (acts, dst) in enumerate(((gat, gg_hbm), (uat, ug_hbm))):
        for at, n in cut(HID):
            v = mm(acts[at : at + n], tc[...].reshape(1024, W)) * (p_x / TOP)
            grads[i, at : at + n] = (turn_cols(v, h128, 2) * R128).astype(bf16)
        store(grads.at[i], dst)
    v = o_part[7, x]
    net.wait(o_cross, oxr.at[pl.ds(1, NX - 1)])
    for j in range(1, NX):
        v = v + oxr[j].astype(f32)
    small[0] = (v * (p_h * p_d / (TOP * TOP))).astype(bf16)
    store(small.at[0], out_hbm)
    v = izf[0]
    net.count(izs.at[0], NZ - 1)
    net.wait(i_owner, izr.at[pl.ds(1, NZ - 1)])
    for d in range(1, NZ):
        v = v + izr[d].astype(f32)
    small[1] = (turn_cols(v, h128, 3) * R128).astype(bf16)
    store(small.at[1], ig_hbm)
    net.wait_sent(unread)
    for copy in stores:
        copy.wait()


def hand_over(*refs):
    n = len(refs) // 3
    given, sems = refs[: 2 * n], refs[-1]
    kept = refs[2 * n : 3 * n]
    copies = []
    for i in range(n):
        copies.append(pltpu.make_async_copy(given[i], kept[i], sems.at[i]))
        copies[i].start()
    outs = []
    for i in range(n):
        copies[i].wait()
        outs.append(pltpu.make_async_copy(kept[i], given[n + i], sems.at[n + i]))
        outs[i].start()
    for out in outs:
        out.wait()


def shards(tokens, cotangent, gate_weight, up_weight, down_weight):
    def vm(shape, dtype):
        return pltpu.VMEM(shape, dtype)

    part = (NZ, NX, ROWS, W)
    scratch = [
        vm((256, 256), bf16), vm((256, 256), bf16), vm((3, HID, W), bf16),
        vm(part, bf16), vm(part, bf16), vm((8, 128, W), bf16),
        vm((HID, W), f32), vm((HID, W), f32), vm((HID, W), f32),
        vm((HID, W), bf16), vm((HID, W), bf16), vm((HID, W), bf16),
        vm((3, 8, 128), f32), vm((17, 8, 128), f32), vm((3, 8, 128), f32), vm((17, 8, 128), f32),
        vm((8, 128), f32), vm((8, 128), f32),
        vm((4, 128, PAIR), f32), vm((4, 128, PAIR), f32), vm((4, 128, PAIR), f32),
        vm((6, 96, PAIR), bf16), vm((2, 96, PAIR), bf16), vm((2, 2, 96, PAIR), bf16),
        vm((4, 64, PAIR), f32), vm((4, 64, PAIR), f32), vm((4, 64, PAIR), f32),
        vm((6, 32, PAIR), bf16), vm((2, 32, PAIR), bf16), vm((2, 2, 32, PAIR), bf16),
        vm((NY, NC, 64, PAIR), bf16), vm((NY, NC, 128, PAIR), bf16), vm((8, 64, PAIR), f32),
        vm((HID, 1024), bf16), vm((HID, 1024), bf16), vm((HID, 1024), bf16),
        vm(part, f32), vm((2, 4, NX, ROWS, W), bf16), vm((2, 4, NX, ROWS, W), bf16),
        vm((NX, ROWS, W), bf16), vm((NX, ROWS, W), bf16),
        vm(part, f32), vm((8, 3, ROWS, W), bf16), vm((8, ROWS, W), bf16), vm((8, 2, ROWS, W), bf16),
        vm((NZ, ROWS, W), f32), vm((NZ, ROWS, W), bf16), vm((NZ, ROWS, W), bf16),
        vm((2, ROWS, W), bf16), vm((3, HID, W), bf16), vm((MOST_SENT, 8, 128), f32),
        pltpu.SemaphoreType.DMA((N_PHASES,)), pltpu.SemaphoreType.DMA((N_SEMS,)), pltpu.SemaphoreType.DMA((8,)),
    ]
    vmem = pl.BlockSpec(memory_space=pltpu.VMEM)
    anywhere = pl.BlockSpec(memory_space=pl.ANY)
    shapes = [jax.ShapeDtypeStruct((HID, W), bf16)] * 3 + [jax.ShapeDtypeStruct((ROWS, W), bf16)] * 2
    results = pl.pallas_call(
        kernel,
        out_shape=shapes,
        in_specs=[vmem] * 2 + [anywhere] * 3,
        out_specs=[anywhere] * 5,
        scratch_shapes=scratch,
        compiler_params=pltpu.CompilerParams(
            collective_id=0, has_side_effects=True, vmem_limit_bytes=60 * 1024 * 1024
        ),
    )(tokens, cotangent, gate_weight.T, up_weight.T, down_weight)
    gg, ug, dg, out, ig = pl.pallas_call(
        hand_over,
        out_shape=shapes,
        in_specs=[anywhere] * 5,
        out_specs=[anywhere] * 5,
        scratch_shapes=[vm(s.shape, s.dtype) for s in shapes] + [pltpu.SemaphoreType.DMA((10,))],
    )(*results)
    return out, ig, gg.T, ug.T, dg


def solution(mesh):
    fine = Mesh(mesh.devices.reshape(NY, NC, NZ, NX), GX + GY)
    specs = (P(GY, GX), P(GY, GX), P(GX, GY), P(GX, GY), P(GY, GX))
    return jax.shard_map(
        shards, mesh=fine, in_specs=specs, out_specs=specs, check_vma=False
    )
```

```python
import functools

import jax
import jax.numpy as jnp
from jax import lax
from jax.experimental import pallas as pl
from jax.experimental.pallas import tpu as pltpu
from jax.sharding import Mesh
from jax.sharding import PartitionSpec as P

GY = ("gy_0", "gy_1")
GX = ("gx_0", "gx_1")
NY, NC, NZ, NX = 4, 2, 8, 4
MESH = pl.DeviceIdType.MESH
f32 = jnp.float32
bf16 = jnp.bfloat16

TOP = 448.0
TINY = 1e-6
ROWS = 32
W = 512
HID = 448
PAIR = 2 * HID
R128 = 128 ** -0.5
R64 = 64 ** -0.5


def mm(a, b):
    return lax.dot_general(a, b, (((1,), (0,)), ((), ())), preferred_element_type=f32)


def mm_t(a, b):
    return lax.dot_general(a, b, (((1,), (1,)), ((), ())), preferred_element_type=f32)


def table(size, block):
    i = lax.broadcasted_iota(jnp.int32, (size, size), 0)
    j = lax.broadcasted_iota(jnp.int32, (size, size), 1)
    v = i & j & (block - 1)
    v = v ^ (v >> 4)
    v = v ^ (v >> 2)
    v = v ^ (v >> 1)
    sign = 1 - 2 * (v & 1)
    same = (i & ~(block - 1)) == (j & ~(block - 1))
    return jnp.where(same, sign, 0).astype(f32).astype(bf16)


def cut(n):
    at = 0
    while at < n:
        yield at, min(256, n - at)
        at += 256


def split(v, terms):
    parts = []
    for _ in range(terms):
        p = v.astype(bf16)
        parts.append(p)
        v = v - p.astype(f32)
    return parts


def turn_cols(v, h, terms=1):
    parts = split(v, terms) if terms > 1 else [v]
    outs = []
    for at, n in cut(v.shape[1]):
        outs.append(sum(mm(p[:, at : at + n], h[:n, :n]) for p in parts))
    return jnp.concatenate(outs, axis=1)


def encode(v, dst):
    hi = v.astype(bf16)
    dst[0:64] = hi
    hi = hi.astype(f32)
    unit = jnp.abs(hi) * (2.0**-8 / 7.0)
    n = jnp.where(unit > 0, (v - hi) / jnp.where(unit > 0, unit, 1.0), 0.0)
    n = jnp.clip(jnp.floor(n + 0.5), -7.0, 7.0) + 7.0
    dst[64:96] = (n[0:32] * 15.0 + n[32:64]).astype(bf16)


def decode(src):
    hi = src[0:64].astype(f32)
    code = src[64:96].astype(f32)
    first = jnp.floor((code + 0.5) * (1.0 / 15.0))
    n = jnp.concatenate([first, code - first * 15.0], axis=0) - 7.0
    return hi + n * (jnp.abs(hi) * (2.0**-8 / 7.0))


class Net:
    def __init__(self, send, recv):
        self.send_sems, self.recv_sems = send, recv
        self.n = self.phase = 0
        self.sent = [0] * N_PHASES

    def sem(self):
        self.n += 1
        return self.n - 1

    def copy(self, src, dst, sem, **dev):
        names = {"y": "gx_0", "c": "gx_1", "z": "gy_0", "x": "gy_1"}
        return pltpu.make_async_remote_copy(
            src_ref=src,
            dst_ref=dst,
            send_sem=self.send_sems.at[self.phase],
            recv_sem=self.recv_sems.at[sem],
            device_id={names[k]: v for k, v in dev.items()},
            device_id_type=MESH,
        )

    def count(self, src, copies=1):
        size = copies * src.dtype.itemsize
        for n in src.shape:
            size *= n
        self.sent[self.phase] += size

    def send(self, src, dst, sem=None, **dev):
        d = self.copy(src, dst, self.sem() if sem is None else sem, **dev)
        d.start()
        self.count(src)
        return d

    def wait(self, sem, ref):
        self.copy(ref, ref, sem, c=1 - lax.axis_index("gx_1")).wait_recv()

    def wait_sent(self, ref):
        for self.phase in range(N_PHASES):
            part = ref.at[pl.ds(0, self.sent[self.phase] // 4096)]
            self.copy(part, part, 0, c=1 - lax.axis_index("gx_1")).wait_send()


class Peaks:
    def __init__(self, net, src, buf, me):
        self.net, self.src, self.buf = net, src, buf
        self.y, self.c, self.z, self.x = me

    def start(self, v):
        self.src[0] = v
        self.sem = self.net.sem()
        for j in range(1, 8):
            dy, dc = j // 2, j % 2
            self.net.send(
                self.src.at[0], self.buf.at[j - 1], self.sem, y=(self.y + dy) % NY, c=(self.c + dc) % NC
            )

    def gathered(self, level, at, n):
        self.net.wait(self.sem, self.buf.at[pl.ds(at, n)])
        v = self.src[level]
        for j in range(n):
            v = jnp.maximum(v, self.buf[at + j])
        return v

    def second(self):
        self.src[1] = self.gathered(0, 0, 7)
        self.sem = self.net.sem()
        for j in range(1, NX):
            self.net.send(self.src.at[1], self.buf.at[6 + j], self.sem, x=(self.x + j) % NX)

    def third(self):
        self.src[2] = self.gathered(1, 7, 3)
        self.sem = self.net.sem()
        for j in range(1, NZ):
            self.net.send(self.src.at[2], self.buf.at[9 + j], self.sem, z=(self.z + j) % NZ)

    def result(self):
        return self.gathered(2, 10, 7)


class ZX:
    def __init__(self, net, own, buf, z, x):
        self.net, self.own, self.buf, self.z, self.x = net, own, buf, z, x
        self.came, self.crossed = {}, {}
        self.far, self.relays = net.sem(), net.sem()

    def at(self, d):
        return (self.z + d + NZ) % NZ

    def start(self):
        for d in (1, -1, 2, -2):
            self.came[-d] = self.net.send(self.own, self.buf.at[self.z, self.x], z=self.at(d))

    def forward(self, d):
        self.came[d].wait_recv()
        to = self.at(2 if d < 0 else -2)
        block = self.buf.at[self.at(d), self.x]
        if abs(d) == 1:
            self.came[3 * d] = self.net.send(block, block, z=to)
        else:
            half = self.buf.at[self.at(d), self.x, pl.ds(0 if d < 0 else 16, 16)]
            self.net.send(half, half, self.far, z=to)

    def cross(self, d):
        b = self.at(d)
        src = self.buf.at[b, self.x] if d else self.own
        if abs(d) == 3:
            self.came[d].wait_recv()
        if d == 4:
            self.net.wait(self.far, self.buf.at[0, 0])
        self.crossed[d] = self.net.sem()
        for k in (1, 3):
            self.net.send(src, self.buf.at[b, self.x], self.crossed[d], x=(self.x + k) % NX)

    def relay(self, d):
        b, xp, xm = self.at(d), (self.x + 1) % NX, (self.x + 3) % NX
        self.net.wait(self.crossed[d], self.buf.at[0, pl.ds(0, 2)])
        lo = self.buf.at[b, xm, pl.ds(0, 16)]
        self.net.send(lo, lo, self.relays, x=xp)
        hi = self.buf.at[b, xp, pl.ds(16, 16)]
        self.net.send(hi, hi, self.relays, x=xm)

    def done(self):
        self.net.wait(self.relays, self.buf.at[pl.ds(0, 2)])


class Gather:
    def __init__(self, net, buf, half, y, c, together):
        self.net, self.buf, self.half, self.y, self.c = net, buf, half, y, c
        self.yp, self.ym, self.y2 = (y + 1) % NY, (y + 3) % NY, (y + 2) % NY
        self.pair = net.sem() if together else None
        self.rest = net.sem()

    def part(self, y, i):
        return self.buf.at[y, self.c, pl.ds(i * self.half, self.half)]

    def to_pair(self, y):
        return self.net.send(self.buf.at[y, self.c], self.buf.at[y, self.c], self.pair, c=1 - self.c)

    def start(self):
        send, y = self.net.send, self.y
        self.p0 = send(self.part(y, 0), self.part(y, 0), y=self.yp)
        self.m1 = send(self.part(y, 1), self.part(y, 1), y=self.ym)
        self.own = self.to_pair(y)

    def start_rest(self):
        send, y = self.net.send, self.y
        self.p1 = send(self.part(y, 1), self.part(y, 1), y=self.yp)
        self.m0 = send(self.part(y, 0), self.part(y, 0), y=self.ym)

    def relay(self):
        send = self.net.send
        self.p0.wait_recv()
        send(self.part(self.ym, 0), self.part(self.ym, 0), self.rest, y=self.yp)
        self.m1.wait_recv()
        send(self.part(self.yp, 1), self.part(self.yp, 1), self.rest, y=self.ym)

    def share(self):
        self.p1.wait_recv()
        self.fp = self.to_pair(self.ym)
        self.m0.wait_recv()
        self.fm = self.to_pair(self.yp)

    def last(self):
        self.net.wait(self.rest, self.buf.at[0, 0])
        self.f2 = self.to_pair(self.y2)

    def done(self):
        self.net.wait(self.pair, self.buf.at[:, 0])


N_SEMS = 118
N_PHASES = 5
MOST_SENT = 1280
RELATIVE = (3, -3, 2, -2, 1, -1, 4, 0)


def kernel(
    tok, cot, wg_hbm, wu_hbm, wd_hbm,
    gg_hbm, ug_hbm, dg_hbm, out_hbm, ig_hbm,
    h128, h64, wts, t_all, c_all, tc, rg, ru, rd, cg, cu, cd,
    pk_src, pk_buf, ph_src, ph_buf, pk, ph,
    dsrc, drecv, acc, ysrc, yrel, yfin, esrc, erecv, eacc, bsrc, brel, bfin,
    h_all, a_all, hrot, cht, gat, uat,
    o_part, osrc, orecv, oxs, oxr, lsrc, lrel, lfin, lzs, lzr,
    i_part, isrc, irel, ifin, izf, izs, izr,
    small, grads, unread,
    ssem, rsem, lsem,
):
    y = lax.axis_index("gx_0")
    c = lax.axis_index("gx_1")
    z = lax.axis_index("gy_0")
    x = lax.axis_index("gy_1")
    pc = 1 - c
    net = Net(ssem, rsem)
    send = net.send
    yp, ym, y2 = (y + 1) % NY, (y + 3) % NY, (y + 2) % NY
    xp, xm, x2 = (x + 1) % NX, (x + 3) % NX, (x + 2) % NX
    zp, zm = (z + 1) % NZ, (z + 7) % NZ

    def zat(d):
        return (z + d + NZ) % NZ

    barrier = pltpu.get_barrier_semaphore()
    for j in range(1, 8):
        pl.semaphore_signal(
            barrier, inc=1, device_id={"gx_0": (y + j // 2) % NY, "gx_1": (c + j % 2) % NC},
            device_id_type=MESH,
        )
    for j in range(1, NX):
        pl.semaphore_signal(barrier, inc=1, device_id={"gy_1": (x + j) % NX}, device_id_type=MESH)
    for j in range(1, NZ):
        pl.semaphore_signal(barrier, inc=1, device_id={"gy_0": (z + j) % NZ}, device_id_type=MESH)
    loads = [
        pltpu.make_async_copy(w, wts.at[i], lsem.at[i]) for i, w in enumerate((wg_hbm, wu_hbm, wd_hbm))
    ]
    for load in loads:
        load.start()
    h128[...] = table(256, 128)
    h64[...] = table(256, 64)
    t_all[z, x] = tok[...]
    c_all[z, x] = cot[...]
    for load in loads:
        load.wait()

    def rotate_weights():
        rg[...] = turn_cols(wts[0], h128) * R128
        ru[...] = turn_cols(wts[1], h128) * R128
        for at, n in cut(HID):
            rd[at : at + n] = mm(h64[:n, :n], wts[2, at : at + n]) * R64

    p_x = jnp.max(jnp.abs(turn_cols(tok[...], h128))) * R128
    rotate_weights()
    p_g = jnp.max(jnp.abs(rg[...]))
    p_u = jnp.max(jnp.abs(ru[...]))
    p_d = jnp.max(jnp.abs(rd[...]))
    row = lax.broadcasted_iota(jnp.int32, (8, 128), 0)
    own_peaks = jnp.where(row == 0, p_x, jnp.where(row == 1, p_g, jnp.where(row == 2, p_u, p_d)))
    pl.semaphore_wait(barrier, 7 + 3 + 7)

    T = ZX(net, tok, t_all, z, x)
    C = ZX(net, cot, c_all, z, x)
    peaks = Peaks(net, pk_src, pk_buf, (y, c, z, x))
    T.start()
    peaks.start(own_peaks)
    T.cross(0)
    T.forward(1)
    T.forward(-1)
    peaks.second()
    T.cross(1)
    T.cross(-1)
    for d in (2, -2):
        T.forward(d)
        T.cross(d)
    T.relay(0)
    net.phase = 1
    C.start()
    T.relay(1)
    T.relay(-1)
    T.cross(3)
    T.cross(-3)
    T.cross(4)
    T.relay(2)
    T.relay(-2)
    peaks.third()
    for d in (1, -1, 2, -2):
        C.forward(d)
    T.relay(3)
    T.relay(-3)
    T.relay(4)
    for d in (0, 1, -1, 2, -2):
        C.cross(d)
    pk[...] = peaks.result()
    inv_x = 1.0 / (pk[0:1, 0:1] + TINY)
    cg[...] = (TOP * jnp.tanh(rg[...] * (1.0 / (pk[1:2, 0:1] + TINY)))).astype(bf16)
    cu[...] = (TOP * jnp.tanh(ru[...] * (1.0 / (pk[2:3, 0:1] + TINY)))).astype(bf16)
    T.done()

    def gate_up(k, dst):
        t = turn_cols(t_all[k].reshape(4 * ROWS, W), h128)
        t = (TOP * jnp.tanh(t * (R128 * inv_x))).astype(bf16)
        tc[k] = t
        dst[:, 0:HID] = mm_t(t, cg[...])
        dst[:, HID:PAIR] = mm_t(t, cu[...])

    order = [y2, yp, ym, y]
    dh, eh = {}, {}

    def pair_part(i):
        gate_up(order[i] * 2 + pc, dsrc.at[i])
        dh[i] = send(dsrc.at[i], drecv.at[i], c=pc)

    def own_part(i):
        gate_up(order[i] * 2 + c, acc.at[i])

    def q(i, at):
        return acc[i, at : at + 64] + drecv[i, at : at + 64]

    def put(slot, v, dst, sem=None, **dev):
        encode(v, ysrc.at[slot])
        return send(ysrc.at[slot], dst, sem, **dev)

    net.phase = 2
    y_fin, b_fin = net.sem(), net.sem()
    pair_part(0)
    pair_part(1)
    own_part(0)
    C.cross(3)
    C.cross(-3)
    C.cross(4)
    dh[0].wait_recv()
    relp = put(0, q(0, 0), yrel.at[0], y=yp)
    relm = put(1, q(0, 64), yrel.at[1], y=ym)
    own_part(1)
    pair_part(2)
    C.relay(0)
    C.relay(1)
    C.relay(-1)
    own_part(2)
    dh[1].wait_recv()
    put(2, q(1, 64), yfin.at[0, 1], y_fin, y=yp)
    dh[2].wait_recv()
    put(3, q(2, 0), yfin.at[1, 0], y_fin, y=ym)
    C.relay(2)
    C.relay(-2)
    cd[...] = (TOP * jnp.tanh(rd[...] * (1.0 / (pk[3:4, 0:1] + TINY)))).astype(bf16)
    pair_part(3)
    C.relay(3)
    C.relay(-3)
    C.relay(4)
    relp.wait_recv()
    put(4, q(1, 0) + decode(yrel.at[0]), yfin.at[0, 0], y_fin, y=yp)
    relm.wait_recv()
    put(5, q(2, 64) + decode(yrel.at[1]), yfin.at[1, 1], y_fin, y=ym)
    own_part(3)
    C.done()

    def back(k, dst):
        b = mm_t(c_all[k].reshape(4 * ROWS, W), cd[...])
        dst[:, 0:HID] = b[0:64]
        dst[:, HID:PAIR] = b[64:128]

    def e(i, at):
        return eacc[i, at : at + 32] + erecv[i, at : at + 32]

    def put_b(slot, v, dst, sem=None, **dev):
        bsrc[slot] = v.astype(bf16)
        return send(bsrc.at[slot], dst, sem, **dev)

    for i in range(4):
        back(order[i] * 2 + pc, esrc.at[i])
        eh[i] = send(esrc.at[i], erecv.at[i], c=pc)
    for i in range(4):
        back(order[i] * 2 + c, eacc.at[i])
        if i == 0:
            eh[0].wait_recv()
            brp = put_b(0, e(0, 0), brel.at[0], y=yp)
            brm = put_b(1, e(0, 32), brel.at[1], y=ym)
    eh[1].wait_recv()
    put_b(2, e(1, 32), bfin.at[0, 1], b_fin, y=yp)
    eh[2].wait_recv()
    put_b(3, e(2, 0), bfin.at[1, 0], b_fin, y=ym)

    p_x, p_g, p_u, p_d = (pk[i : i + 1, 0:1] for i in range(4))

    blocks = [(y, c), (y, pc), (ym, c), (yp, c), (ym, pc), (yp, pc), (y2, c), (y2, pc)]
    ir = {}
    i_fin = [net.sem() for _ in range(8)]
    i_owner = net.sem()

    def i_block(n):
        yy, cc = blocks[n]
        g = a_all[yy, cc, :, 0:HID]
        u = a_all[yy, cc, :, HID:PAIR]
        v = mm(g, cg[...]) * (p_g / TOP) + mm(u, cu[...]) * (p_u / TOP)
        i_part[n] = v.reshape(NX, ROWS, W)
        isrc[n, 0] = i_part[n, x2].astype(bf16)
        if n % 2 == 0:
            ir[n] = send(isrc.at[n, 0], irel.at[n], x=xp)
            isrc[n, 2] = i_part[n, xm].astype(bf16)
            send(isrc.at[n, 2], ifin.at[n, 1], i_fin[n], x=xm)
        else:
            ir[n] = send(isrc.at[n, 0], irel.at[n], x=xm)
            isrc[n, 1] = i_part[n, xp].astype(bf16)
            send(isrc.at[n, 1], ifin.at[n, 0], i_fin[n], x=xp)
        lanes = pl.ds(pl.multiple_of((yy * 2 + cc) * 128, 128), 128)
        gat[:, lanes] = g.T
        uat[:, lanes] = u.T

    def i_relay(n):
        ir[n].wait_recv()
        if n % 2 == 0:
            isrc[n, 1] = (i_part[n, xp] + irel[n].astype(f32)).astype(bf16)
            send(isrc.at[n, 1], ifin.at[n, 0], i_fin[n], x=xp)
        else:
            isrc[n, 2] = (i_part[n, xm] + irel[n].astype(f32)).astype(bf16)
            send(isrc.at[n, 2], ifin.at[n, 1], i_fin[n], x=xm)

    def i_final(n):
        yy, cc = blocks[n]
        net.wait(i_fin[n], ifin.at[n])
        k = yy * 2 + cc
        d = (k + NZ - z) % NZ
        v = i_part[n, x] + ifin[n, 0].astype(f32) + ifin[n, 1].astype(f32)
        izf[d] = v
        izs[d] = v.astype(bf16)

        @pl.when(d != 0)
        def _():
            net.copy(izs.at[d], izr.at[d], i_owner, z=k).start()

    dh[3].wait_recv()
    net.wait(y_fin, yfin)
    for i in range(2):
        acc[3, 64 * i : 64 * i + 64] = q(3, 64 * i) + decode(yfin.at[0, i]) + decode(yfin.at[1, i])
    gate = acc[3, :, 0:HID] * (p_x * p_g / (TOP * TOP))
    up = acc[3, :, HID:PAIR] * (p_x * p_u / (TOP * TOP))
    s = jax.nn.sigmoid(gate)
    hid = (gate * s * up).astype(bf16)
    h_all[y, c, :, 0:HID] = hid[0:64]
    h_all[y, c, :, HID:PAIR] = hid[64:128]
    hidp = Peaks(net, ph_src, ph_buf, (y, c, z, x))

    def turn_hidden(yy, cc):
        hrot[yy * 2 + cc] = turn_cols(h_all[yy, cc], h64) * R64

    turn_hidden(y, c)
    p_h = jnp.max(jnp.abs(hrot[y * 2 + c]))
    hidp.start(jnp.full((8, 128), p_h, f32))
    net.phase = 3
    H = Gather(net, h_all, 32, y, c, True)
    H.start()
    brp.wait_recv()
    put_b(4, e(1, 0) + brel[0].astype(f32), bfin.at[0, 0], b_fin, y=yp)
    brm.wait_recv()
    put_b(5, e(2, 32) + brel[1].astype(f32), bfin.at[1, 1], b_fin, y=ym)
    H.start_rest()
    hidp.second()
    H.relay()
    eh[3].wait_recv()
    net.wait(b_fin, bfin)
    b = jnp.concatenate(
        [e(3, 32 * i) + bfin[0, i].astype(f32) + bfin[1, i].astype(f32) for i in range(2)], axis=0
    )
    b = turn_cols(b * (p_d / TOP), h64, 3) * R64
    hg = jnp.concatenate([b[:, 0:HID], b[:, HID:PAIR]], axis=0)
    a_all[y, c, :, 0:HID] = (hg * up * s * (1.0 + gate * (1.0 - s))).astype(bf16)
    a_all[y, c, :, HID:PAIR] = (hg * gate * s).astype(bf16)
    G = Gather(net, a_all, 64, y, c, False)
    G.start()
    G.start_rest()
    H.share()
    hidp.third()
    H.last()
    for yy in (ym, yp, y2):
        turn_hidden(yy, c)
    H.done()
    for yy in (y, ym, yp, y2):
        turn_hidden(yy, pc)
    net.phase = 4
    i_block(0)
    ph[...] = hidp.result()
    p_h = ph[0:1, 0:1]
    inv_h = 1.0 / (p_h + TINY)

    def o_block(d):
        k = zat(d)
        v = (TOP * jnp.tanh(hrot[k] * inv_h)).astype(bf16)
        v = jnp.concatenate([v[:, 0:HID], v[:, HID:PAIR]], axis=0)
        cht[:, pl.ds(pl.multiple_of(k * 128, 128), 128)] = v.T
        o_part[RELATIVE.index(d)] = mm(v, cd[...]).reshape(NX, ROWS, W)

    left_r = {}
    left_fin = [net.sem() for _ in range(4)]
    left_owner = net.sem()

    def left_send(g, way, dst, sem=None):
        to = xp if way == 1 else xm
        return send(lsrc.at[g, 0 if sem is None else way], dst, sem, x=to)

    def left_start(g):
        way = 1 if g % 2 == 0 else 2
        for i in range(2):
            lsrc[g, 0, i] = o_part[2 * g + i, x2, :, 0:256].astype(bf16)
        left_r[g] = left_send(g, way, lrel.at[g])
        for i in range(2):
            lsrc[g, 3 - way, i] = o_part[2 * g + i, xp if way == 2 else xm, :, 0:256].astype(bf16)
        left_send(g, 3 - way, lfin.at[g, 2 - way], left_fin[g])

    def left_relay(g):
        way = 1 if g % 2 == 0 else 2
        left_r[g].wait_recv()
        for i in range(2):
            v = o_part[2 * g + i, xp if way == 1 else xm, :, 0:256] + lrel[g, i].astype(f32)
            lsrc[g, way, i] = v.astype(bf16)
        left_send(g, way, lfin.at[g, way - 1], left_fin[g])

    def left_final(g):
        net.wait(left_fin[g], lfin.at[g])
        for i in range(2):
            n = 2 * g + i
            v = o_part[n, x, :, 0:256] + lfin[g, 0, i].astype(f32) + lfin[g, 1, i].astype(f32)
            if n == 7:
                o_part[7, x, :, 0:256] = v
            else:
                lzs[n] = v.astype(bf16)
                send(lzs.at[n], lzr.at[n], left_owner, z=zat(RELATIVE[n]))

    op, om = {}, {}
    o_last, o_cross = net.sem(), net.sem()

    def o_ring(s):
        for side, d, handles, dev in ((0, 4 - s, op, zp), (1, s - 4, om, zm)):
            i = RELATIVE.index(4 if s == 0 else d)
            for j in (2, 3, 0, 1) if side == 0 else (0, 1, 2, 3):
                if s == 0 and (j < 2) != (side == 0):
                    continue
                v = o_part[i, j, :, 256:512]
                if (s - 1, j) in handles:
                    handles[s - 1, j].wait_recv()
                    v = v + orecv[side, s - 1, j].astype(f32)
                osrc[side, s, j] = v.astype(bf16)
                sem = o_last if s == 3 else None
                handles[s, j] = send(osrc.at[side, s, j], orecv.at[side, s, j], sem, z=dev)

    o_block(4)
    o_ring(0)
    G.relay()
    o_block(3)
    o_block(-3)
    left_start(0)
    o_block(2)
    o_block(-2)
    left_start(1)
    G.own.wait_recv()
    i_block(1)
    o_ring(1)
    G.share()
    o_block(1)
    o_block(-1)
    left_start(2)
    o_block(0)
    left_start(3)
    left_relay(0)
    left_relay(1)
    i_relay(0)
    i_relay(1)
    i_block(2)
    i_block(3)
    G.last()
    G.fp.wait_recv()
    i_block(4)
    G.fm.wait_recv()
    i_block(5)
    o_ring(2)
    i_block(6)
    G.f2.wait_recv()
    i_block(7)
    left_relay(2)
    left_relay(3)
    left_final(0)
    left_final(1)
    i_relay(2)
    i_relay(3)
    o_ring(3)
    i_final(0)
    i_final(1)
    i_relay(4)
    i_relay(5)
    left_final(2)
    left_final(3)
    i_relay(6)
    i_relay(7)
    i_final(2)
    i_final(3)

    stores = []

    def store(src, dst):
        copy = pltpu.make_async_copy(src, dst, lsem.at[3 + len(stores)])
        copy.start()
        stores.append(copy)

    def weight_grad(i, acts, dst):
        for at, n in cut(HID):
            v = mm(acts[at : at + n], tc[...].reshape(1024, W)) * (p_x / TOP)
            grads[i, at : at + n] = (turn_cols(v, h128, 2) * R128).astype(bf16)
        store(grads.at[i], dst)

    net.wait(o_last, orecv.at[:, 3])
    for j in range(NX):
        v = o_part[7, j, :, 256:512] + orecv[0, 3, j].astype(f32) + orecv[1, 3, j].astype(f32)
        o_part[7, j, :, 256:512] = v
        oxs[j] = v.astype(bf16)
    for j in range(1, NX):
        send(oxs.at[(x + j) % NX], oxr.at[j], o_cross, x=(x + j) % NX)
    for at, n in cut(HID):
        v = mm(cht[at : at + n], c_all[...].reshape(1024, W)) * (p_h / TOP)
        grads[2, at : at + n] = (sum(mm(h64[:n, :n], p) for p in split(v, 2)) * R64).astype(bf16)
    store(grads.at[2], dg_hbm)
    i_final(4)
    i_final(5)
    weight_grad(0, gat, gg_hbm)
    i_final(6)
    i_final(7)
    weight_grad(1, uat, ug_hbm)
    scale = p_h * p_d / (TOP * TOP)
    net.wait(o_cross, oxr.at[pl.ds(1, NX - 1)])
    v = o_part[7, x, :, 256:512]
    for j in range(1, NX):
        v = v + oxr[j].astype(f32)
    small[0, :, 256:512] = (v * scale).astype(bf16)
    net.wait(left_owner, lzr)
    v = o_part[7, x, :, 0:256]
    for n in range(7):
        v = v + lzr[n].astype(f32)
    small[0, :, 0:256] = (v * scale).astype(bf16)
    store(small.at[0], out_hbm)
    v = izf[0]
    net.count(izs.at[0], NZ - 1)
    net.wait(i_owner, izr.at[pl.ds(1, NZ - 1)])
    for d in range(1, NZ):
        v = v + izr[d].astype(f32)
    small[1] = (turn_cols(v, h128, 3) * R128).astype(bf16)
    store(small.at[1], ig_hbm)
    net.wait_sent(unread)
    for copy in stores:
        copy.wait()


def hand_over(*refs):
    n = len(refs) // 3
    given, sems = refs[: 2 * n], refs[-1]
    kept = refs[2 * n : 3 * n]
    copies = []
    for i in range(n):
        copies.append(pltpu.make_async_copy(given[i], kept[i], sems.at[i]))
        copies[i].start()
    outs = []
    for i in range(n):
        copies[i].wait()
        outs.append(pltpu.make_async_copy(kept[i], given[n + i], sems.at[n + i]))
        outs[i].start()
    for out in outs:
        out.wait()


def shards(tokens, cotangent, gate_weight, up_weight, down_weight):
    def vm(shape, dtype):
        return pltpu.VMEM(shape, dtype)

    part = (NZ, NX, ROWS, W)
    scratch = [
        vm((256, 256), bf16), vm((256, 256), bf16), vm((3, HID, W), bf16),
        vm(part, bf16), vm(part, bf16), vm((8, 128, W), bf16),
        vm((HID, W), f32), vm((HID, W), f32), vm((HID, W), f32),
        vm((HID, W), bf16), vm((HID, W), bf16), vm((HID, W), bf16),
        vm((3, 8, 128), f32), vm((17, 8, 128), f32), vm((3, 8, 128), f32), vm((17, 8, 128), f32),
        vm((8, 128), f32), vm((8, 128), f32),
        vm((4, 128, PAIR), f32), vm((4, 128, PAIR), f32), vm((4, 128, PAIR), f32),
        vm((6, 96, PAIR), bf16), vm((2, 96, PAIR), bf16), vm((2, 2, 96, PAIR), bf16),
        vm((4, 64, PAIR), f32), vm((4, 64, PAIR), f32), vm((4, 64, PAIR), f32),
        vm((6, 32, PAIR), bf16), vm((2, 32, PAIR), bf16), vm((2, 2, 32, PAIR), bf16),
        vm((NY, NC, 64, PAIR), bf16), vm((NY, NC, 128, PAIR), bf16), vm((8, 64, PAIR), f32),
        vm((HID, 1024), bf16), vm((HID, 1024), bf16), vm((HID, 1024), bf16),
        vm(part, f32), vm((2, 4, NX, ROWS, 256), bf16), vm((2, 4, NX, ROWS, 256), bf16),
        vm((NX, ROWS, 256), bf16), vm((NX, ROWS, 256), bf16),
        vm((4, 3, 2, ROWS, 256), bf16), vm((4, 2, ROWS, 256), bf16), vm((4, 2, 2, ROWS, 256), bf16),
        vm((7, ROWS, 256), bf16), vm((7, ROWS, 256), bf16),
        vm(part, f32), vm((8, 3, ROWS, W), bf16), vm((8, ROWS, W), bf16), vm((8, 2, ROWS, W), bf16),
        vm((NZ, ROWS, W), f32), vm((NZ, ROWS, W), bf16), vm((NZ, ROWS, W), bf16),
        vm((2, ROWS, W), bf16), vm((3, HID, W), bf16), vm((MOST_SENT, 8, 128), f32),
        pltpu.SemaphoreType.DMA((N_PHASES,)), pltpu.SemaphoreType.DMA((N_SEMS,)), pltpu.SemaphoreType.DMA((8,)),
    ]
    vmem = pl.BlockSpec(memory_space=pltpu.VMEM)
    anywhere = pl.BlockSpec(memory_space=pl.ANY)
    shapes = [jax.ShapeDtypeStruct((HID, W), bf16)] * 3 + [jax.ShapeDtypeStruct((ROWS, W), bf16)] * 2
    results = pl.pallas_call(
        kernel,
        out_shape=shapes,
        in_specs=[vmem] * 2 + [anywhere] * 3,
        out_specs=[anywhere] * 5,
        scratch_shapes=scratch,
        compiler_params=pltpu.CompilerParams(
            collective_id=0, has_side_effects=True, vmem_limit_bytes=60 * 1024 * 1024
        ),
    )(tokens, cotangent, gate_weight.T, up_weight.T, down_weight)
    gg, ug, dg, out, ig = pl.pallas_call(
        hand_over,
        out_shape=shapes,
        in_specs=[anywhere] * 5,
        out_specs=[anywhere] * 5,
        scratch_shapes=[vm(s.shape, s.dtype) for s in shapes] + [pltpu.SemaphoreType.DMA((10,))],
    )(*results)
    return out, ig, gg.T, ug.T, dg


def solution(mesh):
    fine = Mesh(mesh.devices.reshape(NY, NC, NZ, NX), GX + GY)
    specs = (P(GY, GX), P(GY, GX), P(GX, GY), P(GX, GY), P(GY, GX))
    return jax.shard_map(
        shards, mesh=fine, in_specs=specs, out_specs=specs, check_vma=False
    )
```

```python
import functools

import jax
import jax.numpy as jnp
from jax import lax
from jax.experimental import pallas as pl
from jax.experimental.pallas import tpu as pltpu
from jax.sharding import Mesh
from jax.sharding import PartitionSpec as P

GY = ("gy_0", "gy_1")
GX = ("gx_0", "gx_1")
NY, NC, NZ, NX = 4, 2, 8, 4
MESH = pl.DeviceIdType.MESH
f32 = jnp.float32
bf16 = jnp.bfloat16

TOP = 448.0
TINY = 1e-6
ROWS = 32
W = 512
HID = 448
PAIR = 2 * HID
R128 = 128 ** -0.5
R64 = 64 ** -0.5


def mm(a, b):
    return lax.dot_general(a, b, (((1,), (0,)), ((), ())), preferred_element_type=f32)


def mm_t(a, b):
    return lax.dot_general(a, b, (((1,), (1,)), ((), ())), preferred_element_type=f32)


def table(size, block):
    i = lax.broadcasted_iota(jnp.int32, (size, size), 0)
    j = lax.broadcasted_iota(jnp.int32, (size, size), 1)
    v = i & j & (block - 1)
    v = v ^ (v >> 4)
    v = v ^ (v >> 2)
    v = v ^ (v >> 1)
    sign = 1 - 2 * (v & 1)
    same = (i & ~(block - 1)) == (j & ~(block - 1))
    return jnp.where(same, sign, 0).astype(f32).astype(bf16)


def cut(n):
    at = 0
    while at < n:
        yield at, min(256, n - at)
        at += 256


def split(v, terms):
    parts = []
    for _ in range(terms):
        p = v.astype(bf16)
        parts.append(p)
        v = v - p.astype(f32)
    return parts


def turn_cols(v, h, terms=1):
    parts = split(v, terms) if terms > 1 else [v]
    outs = []
    for at, n in cut(v.shape[1]):
        outs.append(sum(mm(p[:, at : at + n], h[:n, :n]) for p in parts))
    return jnp.concatenate(outs, axis=1)


def encode(v, dst):
    hi = v.astype(bf16)
    dst[0:64] = hi
    hi = hi.astype(f32)
    unit = jnp.abs(hi) * (2.0**-8 / 7.0)
    n = jnp.where(unit > 0, (v - hi) / jnp.where(unit > 0, unit, 1.0), 0.0)
    n = jnp.clip(jnp.floor(n + 0.5), -7.0, 7.0) + 7.0
    dst[64:96] = (n[0:32] * 15.0 + n[32:64]).astype(bf16)


def decode(src):
    hi = src[0:64].astype(f32)
    code = src[64:96].astype(f32)
    first = jnp.floor((code + 0.5) * (1.0 / 15.0))
    n = jnp.concatenate([first, code - first * 15.0], axis=0) - 7.0
    return hi + n * (jnp.abs(hi) * (2.0**-8 / 7.0))


class Net:
    def __init__(self, send, recv):
        self.send_sems, self.recv_sems = send, recv
        self.n = self.phase = 0
        self.sent = [0] * N_PHASES

    def sem(self):
        self.n += 1
        return self.n - 1

    def copy(self, src, dst, sem, **dev):
        names = {"y": "gx_0", "c": "gx_1", "z": "gy_0", "x": "gy_1"}
        return pltpu.make_async_remote_copy(
            src_ref=src,
            dst_ref=dst,
            send_sem=self.send_sems.at[self.phase],
            recv_sem=self.recv_sems.at[sem],
            device_id={names[k]: v for k, v in dev.items()},
            device_id_type=MESH,
        )

    def count(self, src, copies=1):
        size = copies * src.dtype.itemsize
        for n in src.shape:
            size *= n
        self.sent[self.phase] += size

    def send(self, src, dst, sem=None, **dev):
        d = self.copy(src, dst, self.sem() if sem is None else sem, **dev)
        d.start()
        self.count(src)
        return d

    def wait(self, sem, ref):
        self.copy(ref, ref, sem, c=1 - lax.axis_index("gx_1")).wait_recv()

    def wait_sent(self, ref):
        for self.phase in range(N_PHASES):
            part = ref.at[pl.ds(0, self.sent[self.phase] // 4096)]
            self.copy(part, part, 0, c=1 - lax.axis_index("gx_1")).wait_send()


class Peaks:
    def __init__(self, net, src, buf, me):
        self.net, self.src, self.buf = net, src, buf
        self.y, self.c, self.z, self.x = me

    def start(self, v):
        self.src[0] = v
        self.sem = self.net.sem()
        for j in range(1, 8):
            dy, dc = j // 2, j % 2
            self.net.send(
                self.src.at[0], self.buf.at[j - 1], self.sem, y=(self.y + dy) % NY, c=(self.c + dc) % NC
            )

    def gathered(self, level, at, n):
        self.net.wait(self.sem, self.buf.at[pl.ds(at, n)])
        v = self.src[level]
        for j in range(n):
            v = jnp.maximum(v, self.buf[at + j])
        return v

    def second(self):
        self.src[1] = self.gathered(0, 0, 7)
        self.sem = self.net.sem()
        for j in range(1, NX):
            self.net.send(self.src.at[1], self.buf.at[6 + j], self.sem, x=(self.x + j) % NX)

    def third(self):
        self.src[2] = self.gathered(1, 7, 3)
        self.sem = self.net.sem()
        for j in range(1, NZ):
            self.net.send(self.src.at[2], self.buf.at[9 + j], self.sem, z=(self.z + j) % NZ)

    def result(self):
        return self.gathered(2, 10, 7)


class ZX:
    def __init__(self, net, own, buf, z, x):
        self.net, self.own, self.buf, self.z, self.x = net, own, buf, z, x
        self.came, self.crossed = {}, {}
        self.far, self.relays = net.sem(), net.sem()

    def at(self, d):
        return (self.z + d + NZ) % NZ

    def start(self):
        for d in (1, -1, 2, -2):
            self.came[-d] = self.net.send(self.own, self.buf.at[self.z, self.x], z=self.at(d))

    def forward(self, d):
        self.came[d].wait_recv()
        to = self.at(2 if d < 0 else -2)
        block = self.buf.at[self.at(d), self.x]
        if abs(d) == 1:
            self.came[3 * d] = self.net.send(block, block, z=to)
        else:
            half = self.buf.at[self.at(d), self.x, pl.ds(0 if d < 0 else 16, 16)]
            self.net.send(half, half, self.far, z=to)

    def cross(self, d):
        b = self.at(d)
        src = self.buf.at[b, self.x] if d else self.own
        if abs(d) == 3:
            self.came[d].wait_recv()
        if d == 4:
            self.net.wait(self.far, self.buf.at[0, 0])
        self.crossed[d] = self.net.sem()
        for k in (1, 3):
            self.net.send(src, self.buf.at[b, self.x], self.crossed[d], x=(self.x + k) % NX)

    def relay(self, d):
        b, xp, xm = self.at(d), (self.x + 1) % NX, (self.x + 3) % NX
        self.net.wait(self.crossed[d], self.buf.at[0, pl.ds(0, 2)])
        lo = self.buf.at[b, xm, pl.ds(0, 16)]
        self.net.send(lo, lo, self.relays, x=xp)
        hi = self.buf.at[b, xp, pl.ds(16, 16)]
        self.net.send(hi, hi, self.relays, x=xm)

    def done(self):
        self.net.wait(self.relays, self.buf.at[pl.ds(0, 2)])


class Gather:
    def __init__(self, net, buf, half, y, c, together):
        self.net, self.buf, self.half, self.y, self.c = net, buf, half, y, c
        self.yp, self.ym, self.y2 = (y + 1) % NY, (y + 3) % NY, (y + 2) % NY
        self.pair = net.sem() if together else None
        self.rest = net.sem()

    def part(self, y, i):
        return self.buf.at[y, self.c, pl.ds(i * self.half, self.half)]

    def to_pair(self, y):
        return self.net.send(self.buf.at[y, self.c], self.buf.at[y, self.c], self.pair, c=1 - self.c)

    def start(self):
        send, y = self.net.send, self.y
        self.p0 = send(self.part(y, 0), self.part(y, 0), y=self.yp)
        self.m1 = send(self.part(y, 1), self.part(y, 1), y=self.ym)
        self.own = self.to_pair(y)

    def start_rest(self):
        send, y = self.net.send, self.y
        self.p1 = send(self.part(y, 1), self.part(y, 1), y=self.yp)
        self.m0 = send(self.part(y, 0), self.part(y, 0), y=self.ym)

    def relay(self):
        send = self.net.send
        self.p0.wait_recv()
        send(self.part(self.ym, 0), self.part(self.ym, 0), self.rest, y=self.yp)
        self.m1.wait_recv()
        send(self.part(self.yp, 1), self.part(self.yp, 1), self.rest, y=self.ym)

    def share(self):
        self.p1.wait_recv()
        self.fp = self.to_pair(self.ym)
        self.m0.wait_recv()
        self.fm = self.to_pair(self.yp)

    def last(self):
        self.net.wait(self.rest, self.buf.at[0, 0])
        self.f2 = self.to_pair(self.y2)

    def done(self):
        self.net.wait(self.pair, self.buf.at[:, 0])


N_SEMS = 118
N_PHASES = 5
MOST_SENT = 1280
RELATIVE = (3, -3, 4, 0, 2, -2, 1, -1)


def kernel(
    tok_hbm, cot_hbm, wg_hbm, wu_hbm, wd_hbm,
    gg, ug, dg, out, ig,
    tok, cot, h128, h64, wts, t_all, c_all, tc, rg, ru, rd, cg, cu, cd,
    pk_src, pk_buf, ph_src, ph_buf, pk, ph,
    dsrc, drecv, acc, ysrc, yrel, yfin, esrc, erecv, eacc, bsrc, brel, bfin,
    h_all, a_all, hrot, cht, gat, uat,
    o_part, osrc, orecv, oxs, oxr, lsrc, lrel, lfin, lzs, lzr,
    i_part, isrc, irel, ifin, izf, izs, izr,
    unread,
    ssem, rsem, lsem,
):
    y = lax.axis_index("gx_0")
    c = lax.axis_index("gx_1")
    z = lax.axis_index("gy_0")
    x = lax.axis_index("gy_1")
    pc = 1 - c
    net = Net(ssem, rsem)
    send = net.send
    yp, ym, y2 = (y + 1) % NY, (y + 3) % NY, (y + 2) % NY
    xp, xm, x2 = (x + 1) % NX, (x + 3) % NX, (x + 2) % NX
    zp, zm = (z + 1) % NZ, (z + 7) % NZ

    def zat(d):
        return (z + d + NZ) % NZ

    barrier = pltpu.get_barrier_semaphore()
    for j in range(1, 8):
        pl.semaphore_signal(
            barrier, inc=1, device_id={"gx_0": (y + j // 2) % NY, "gx_1": (c + j % 2) % NC},
            device_id_type=MESH,
        )
    for j in range(1, NX):
        pl.semaphore_signal(barrier, inc=1, device_id={"gy_1": (x + j) % NX}, device_id_type=MESH)
    for j in range(1, NZ):
        pl.semaphore_signal(barrier, inc=1, device_id={"gy_0": (z + j) % NZ}, device_id_type=MESH)
    loads = [
        pltpu.make_async_copy(src, dst, lsem.at[i])
        for i, (src, dst) in enumerate(
            (
                (tok_hbm, tok), (cot_hbm, cot),
                (wg_hbm, wts.at[0]), (wu_hbm, wts.at[1]), (wd_hbm, wts.at[2]),
            )
        )
    ]
    for load in loads:
        load.start()
    h128[...] = table(256, 128)
    h64[...] = table(256, 64)
    for load in loads:
        load.wait()
    t_all[z, x] = tok[...]
    c_all[z, x] = cot[...]

    def rotate_weights():
        rg[...] = turn_cols(wts[0], h128) * R128
        ru[...] = turn_cols(wts[1], h128) * R128
        for at, n in cut(HID):
            rd[at : at + n] = mm(h64[:n, :n], wts[2, at : at + n]) * R64

    p_x = jnp.max(jnp.abs(turn_cols(tok[...], h128))) * R128
    rotate_weights()
    p_g = jnp.max(jnp.abs(rg[...]))
    p_u = jnp.max(jnp.abs(ru[...]))
    p_d = jnp.max(jnp.abs(rd[...]))
    row = lax.broadcasted_iota(jnp.int32, (8, 128), 0)
    own_peaks = jnp.where(row == 0, p_x, jnp.where(row == 1, p_g, jnp.where(row == 2, p_u, p_d)))
    pl.semaphore_wait(barrier, 7 + 3 + 7)

    T = ZX(net, tok, t_all, z, x)
    C = ZX(net, cot, c_all, z, x)
    peaks = Peaks(net, pk_src, pk_buf, (y, c, z, x))
    T.start()
    peaks.start(own_peaks)
    T.cross(0)
    T.forward(1)
    T.forward(-1)
    peaks.second()
    T.cross(1)
    T.cross(-1)
    for d in (2, -2):
        T.forward(d)
        T.cross(d)
    T.relay(0)
    net.phase = 1
    C.start()
    T.relay(1)
    T.relay(-1)
    T.cross(3)
    T.cross(-3)
    T.cross(4)
    T.relay(2)
    T.relay(-2)
    peaks.third()
    for d in (1, -1, 2, -2):
        C.forward(d)
    T.relay(3)
    T.relay(-3)
    T.relay(4)
    for d in (0, 1, -1, 2, -2):
        C.cross(d)
    pk[...] = peaks.result()
    inv_x = 1.0 / (pk[0:1, 0:1] + TINY)
    cg[...] = (TOP * jnp.tanh(rg[...] * (1.0 / (pk[1:2, 0:1] + TINY)))).astype(bf16)
    cu[...] = (TOP * jnp.tanh(ru[...] * (1.0 / (pk[2:3, 0:1] + TINY)))).astype(bf16)
    T.done()

    def gate_up(k, dst):
        t = turn_cols(t_all[k].reshape(4 * ROWS, W), h128)
        t = (TOP * jnp.tanh(t * (R128 * inv_x))).astype(bf16)
        tc[k] = t
        dst[:, 0:HID] = mm_t(t, cg[...])
        dst[:, HID:PAIR] = mm_t(t, cu[...])

    order = [y2, yp, ym, y]
    dh, eh = {}, {}

    def pair_part(i):
        gate_up(order[i] * 2 + pc, dsrc.at[i])
        if i == 0:
            first, last = pl.ds(0, 64), pl.ds(64, 64)
            dh["first"] = send(dsrc.at[0, first], drecv.at[0, first], c=pc)
            dh[0] = send(dsrc.at[0, last], drecv.at[0, last], c=pc)
        else:
            dh[i] = send(dsrc.at[i], drecv.at[i], c=pc)

    def own_part(i):
        gate_up(order[i] * 2 + c, acc.at[i])

    def q(i, at):
        return acc[i, at : at + 64] + drecv[i, at : at + 64]

    def put(slot, v, dst, sem=None, **dev):
        encode(v, ysrc.at[slot])
        return send(ysrc.at[slot], dst, sem, **dev)

    net.phase = 2
    y_fin, b_fin = net.sem(), net.sem()
    pair_part(0)
    pair_part(1)
    own_part(0)
    C.cross(3)
    C.cross(-3)
    C.cross(4)
    dh["first"].wait_recv()
    relp = put(0, q(0, 0), yrel.at[0], y=yp)
    dh[0].wait_recv()
    relm = put(1, q(0, 64), yrel.at[1], y=ym)
    own_part(1)
    pair_part(2)
    C.relay(0)
    C.relay(1)
    C.relay(-1)
    own_part(2)
    dh[1].wait_recv()
    put(2, q(1, 64), yfin.at[0, 1], y_fin, y=yp)
    dh[2].wait_recv()
    put(3, q(2, 0), yfin.at[1, 0], y_fin, y=ym)
    C.relay(2)
    C.relay(-2)
    cd[...] = (TOP * jnp.tanh(rd[...] * (1.0 / (pk[3:4, 0:1] + TINY)))).astype(bf16)
    pair_part(3)
    C.relay(3)
    C.relay(-3)
    C.relay(4)
    relp.wait_recv()
    put(4, q(1, 0) + decode(yrel.at[0]), yfin.at[0, 0], y_fin, y=yp)
    relm.wait_recv()
    put(5, q(2, 64) + decode(yrel.at[1]), yfin.at[1, 1], y_fin, y=ym)
    own_part(3)
    C.done()

    def back(k, dst):
        b = mm_t(c_all[k].reshape(4 * ROWS, W), cd[...])
        dst[:, 0:HID] = b[0:64]
        dst[:, HID:PAIR] = b[64:128]

    def e(i, at):
        return eacc[i, at : at + 32] + erecv[i, at : at + 32]

    def put_b(slot, v, dst, sem=None, **dev):
        bsrc[slot] = v.astype(bf16)
        return send(bsrc.at[slot], dst, sem, **dev)

    for i in range(4):
        back(order[i] * 2 + pc, esrc.at[i])
        eh[i] = send(esrc.at[i], erecv.at[i], c=pc)
    for i in range(4):
        back(order[i] * 2 + c, eacc.at[i])
        if i == 0:
            eh[0].wait_recv()
            brp = put_b(0, e(0, 0), brel.at[0], y=yp)
            brm = put_b(1, e(0, 32), brel.at[1], y=ym)
    eh[1].wait_recv()
    put_b(2, e(1, 32), bfin.at[0, 1], b_fin, y=yp)
    eh[2].wait_recv()
    put_b(3, e(2, 0), bfin.at[1, 0], b_fin, y=ym)

    p_x, p_g, p_u, p_d = (pk[i : i + 1, 0:1] for i in range(4))

    blocks = [(y, c), (y, pc), (ym, c), (yp, c), (ym, pc), (yp, pc), (y2, c), (y2, pc)]
    ir = {}
    i_fin = [net.sem() for _ in range(8)]
    i_owner = net.sem()

    def i_block(n):
        yy, cc = blocks[n]
        g = a_all[yy, cc, :, 0:HID]
        u = a_all[yy, cc, :, HID:PAIR]
        v = mm(g, cg[...]) * (p_g / TOP) + mm(u, cu[...]) * (p_u / TOP)
        i_part[n] = v.reshape(NX, ROWS, W)
        isrc[n, 0] = i_part[n, x2].astype(bf16)
        if n % 2 == 0:
            ir[n] = send(isrc.at[n, 0], irel.at[n], x=xp)
            isrc[n, 2] = i_part[n, xm].astype(bf16)
            send(isrc.at[n, 2], ifin.at[n, 1], i_fin[n], x=xm)
        else:
            ir[n] = send(isrc.at[n, 0], irel.at[n], x=xm)
            isrc[n, 1] = i_part[n, xp].astype(bf16)
            send(isrc.at[n, 1], ifin.at[n, 0], i_fin[n], x=xp)
        lanes = pl.ds(pl.multiple_of((yy * 2 + cc) * 128, 128), 128)
        gat[:, lanes] = g.T
        uat[:, lanes] = u.T

    def i_relay(n):
        ir[n].wait_recv()
        if n % 2 == 0:
            isrc[n, 1] = (i_part[n, xp] + irel[n].astype(f32)).astype(bf16)
            send(isrc.at[n, 1], ifin.at[n, 0], i_fin[n], x=xp)
        else:
            isrc[n, 2] = (i_part[n, xm] + irel[n].astype(f32)).astype(bf16)
            send(isrc.at[n, 2], ifin.at[n, 1], i_fin[n], x=xm)

    def i_final(n):
        yy, cc = blocks[n]
        net.wait(i_fin[n], ifin.at[n])
        k = yy * 2 + cc
        d = (k + NZ - z) % NZ
        v = i_part[n, x] + ifin[n, 0].astype(f32) + ifin[n, 1].astype(f32)
        izf[d] = v
        izs[d] = v.astype(bf16)

        @pl.when(d != 0)
        def _():
            net.copy(izs.at[d], izr.at[d], i_owner, z=k).start()

    dh[3].wait_recv()
    net.wait(y_fin, yfin)
    for i in range(2):
        acc[3, 64 * i : 64 * i + 64] = q(3, 64 * i) + decode(yfin.at[0, i]) + decode(yfin.at[1, i])
    gate = acc[3, :, 0:HID] * (p_x * p_g / (TOP * TOP))
    up = acc[3, :, HID:PAIR] * (p_x * p_u / (TOP * TOP))
    s = jax.nn.sigmoid(gate)
    hid = (gate * s * up).astype(bf16)
    h_all[y, c, :, 0:HID] = hid[0:64]
    h_all[y, c, :, HID:PAIR] = hid[64:128]
    hidp = Peaks(net, ph_src, ph_buf, (y, c, z, x))

    def turn_hidden(yy, cc):
        hrot[yy * 2 + cc] = turn_cols(h_all[yy, cc], h64) * R64

    turn_hidden(y, c)
    p_h = jnp.max(jnp.abs(hrot[y * 2 + c]))
    hidp.start(jnp.full((8, 128), p_h, f32))
    net.phase = 3
    H = Gather(net, h_all, 32, y, c, True)
    H.start()
    brp.wait_recv()
    put_b(4, e(1, 0) + brel[0].astype(f32), bfin.at[0, 0], b_fin, y=yp)
    brm.wait_recv()
    put_b(5, e(2, 32) + brel[1].astype(f32), bfin.at[1, 1], b_fin, y=ym)
    H.start_rest()
    hidp.second()
    H.relay()
    eh[3].wait_recv()
    net.wait(b_fin, bfin)
    b = jnp.concatenate(
        [e(3, 32 * i) + bfin[0, i].astype(f32) + bfin[1, i].astype(f32) for i in range(2)], axis=0
    )
    b = turn_cols(b * (p_d / TOP), h64, 3) * R64
    hg = jnp.concatenate([b[:, 0:HID], b[:, HID:PAIR]], axis=0)
    a_all[y, c, :, 0:HID] = (hg * up * s * (1.0 + gate * (1.0 - s))).astype(bf16)
    a_all[y, c, :, HID:PAIR] = (hg * gate * s).astype(bf16)
    G = Gather(net, a_all, 64, y, c, False)
    G.start()
    G.start_rest()
    net.phase = 4
    i_block(0)
    H.share()
    hidp.third()
    G.own.wait_recv()
    i_block(1)
    H.last()
    for yy in (ym, yp, y2):
        turn_hidden(yy, c)
    H.done()
    for yy in (y, ym, yp, y2):
        turn_hidden(yy, pc)
    G.relay()
    i_relay(0)
    i_relay(1)
    ph[...] = hidp.result()
    p_h = ph[0:1, 0:1]
    inv_h = 1.0 / (p_h + TINY)

    def o_block(d):
        k = zat(d)
        v = (TOP * jnp.tanh(hrot[k] * inv_h)).astype(bf16)
        v = jnp.concatenate([v[:, 0:HID], v[:, HID:PAIR]], axis=0)
        cht[:, pl.ds(pl.multiple_of(k * 128, 128), 128)] = v.T
        o_part[RELATIVE.index(d)] = mm(v, cd[...]).reshape(NX, ROWS, W)

    left_r = {}
    left_fin = [net.sem() for _ in range(4)]
    left_owner, left_mid = net.sem(), net.sem()
    ZERO = RELATIVE.index(0)

    def left_send(g, way, dst, sem=None):
        to = xp if way == 1 else xm
        return send(lsrc.at[g, 0 if sem is None else way], dst, sem, x=to)

    def left_start(g):
        way = 1 if g % 2 == 0 else 2
        for i in range(2):
            lsrc[g, 0, i] = o_part[2 * g + i, x2, :, 0:256].astype(bf16)
        left_r[g] = left_send(g, way, lrel.at[g])
        for i in range(2):
            lsrc[g, 3 - way, i] = o_part[2 * g + i, xp if way == 2 else xm, :, 0:256].astype(bf16)
        left_send(g, 3 - way, lfin.at[g, 2 - way], left_fin[g])

    def left_relay(g):
        way = 1 if g % 2 == 0 else 2
        left_r[g].wait_recv()
        for i in range(2):
            v = o_part[2 * g + i, xp if way == 1 else xm, :, 0:256] + lrel[g, i].astype(f32)
            lsrc[g, way, i] = v.astype(bf16)
        left_send(g, way, lfin.at[g, way - 1], left_fin[g])

    def left_final(g):
        net.wait(left_fin[g], lfin.at[g])
        if g == 2:
            net.wait(left_mid, lzr.at[pl.ds(0, 3)])
        for i in range(2):
            n, d = 2 * g + i, RELATIVE[2 * g + i]
            v = o_part[n, x, :, 0:256] + lfin[g, 0, i].astype(f32) + lfin[g, 1, i].astype(f32)
            if abs(d) == 2:
                v = v + lzr[0 if d > 0 else 1].astype(f32)
                half = lzr[2].astype(f32)
                rows = lax.broadcasted_iota(jnp.int32, (ROWS, 256), 0)
                v = v + jnp.where((rows < 16) if d > 0 else (rows >= 16), half, 0.0)
            if d == 0:
                o_part[n, x, :, 0:256] = v
                continue
            lzs[n] = v.astype(bf16)
            if d == 4:
                for at, to in ((0, 2), (16, -2)):
                    rows = pl.ds(at, 16)
                    send(lzs.at[n, rows], lzr.at[2, rows], left_mid, z=zat(to))
            elif abs(d) == 3:
                send(lzs.at[n], lzr.at[0 if d > 0 else 1], left_mid, z=zat(d // 3))
            else:
                send(lzs.at[n], lzr.at[3 + RELATIVE[4:].index(d)], left_owner, z=zat(d))

    op, om = {}, {}
    o_last, o_cross = net.sem(), net.sem()

    def o_ring(s):
        for side, d, handles, dev in ((0, 4 - s, op, zp), (1, s - 4, om, zm)):
            i = RELATIVE.index(4 if s == 0 else d)
            for j in (2, 3, 0, 1) if side == 0 else (0, 1, 2, 3):
                if s == 0 and (j < 2) != (side == 0):
                    continue
                v = o_part[i, j, :, 256:512]
                if (s - 1, j) in handles:
                    handles[s - 1, j].wait_recv()
                    v = v + orecv[side, s - 1, j].astype(f32)
                osrc[side, s, j] = v.astype(bf16)
                sem = o_last if s == 3 else None
                handles[s, j] = send(osrc.at[side, s, j], orecv.at[side, s, j], sem, z=dev)

    o_block(4)
    o_ring(0)
    o_block(3)
    o_block(-3)
    left_start(0)
    o_block(0)
    left_start(1)
    i_final(0)
    i_final(1)
    o_block(2)
    o_block(-2)
    o_ring(1)
    G.share()
    left_start(2)
    o_block(1)
    o_block(-1)
    left_start(3)
    left_relay(0)
    left_relay(1)
    i_block(2)
    i_block(3)
    G.last()
    G.fp.wait_recv()
    i_block(4)
    G.fm.wait_recv()
    i_block(5)
    o_ring(2)
    i_block(6)
    G.f2.wait_recv()
    i_block(7)
    left_final(0)
    left_final(1)
    i_relay(2)
    i_relay(3)
    left_relay(2)
    left_relay(3)
    o_ring(3)
    i_relay(4)
    i_relay(5)
    i_relay(6)
    i_relay(7)
    i_final(2)
    i_final(3)
    left_final(2)
    left_final(3)

    def weight_grad(acts, dst):
        for at, n in cut(HID):
            v = mm(acts[at : at + n], tc[...].reshape(1024, W)) * (p_x / TOP)
            dst[at : at + n] = (turn_cols(v, h128, 2) * R128).astype(bf16)

    net.wait(o_last, orecv.at[:, 3])
    for j in range(NX):
        v = o_part[ZERO, j, :, 256:512] + orecv[0, 3, j].astype(f32) + orecv[1, 3, j].astype(f32)
        o_part[ZERO, j, :, 256:512] = v
        oxs[j] = v.astype(bf16)
    for j in range(1, NX):
        send(oxs.at[(x + j) % NX], oxr.at[j], o_cross, x=(x + j) % NX)
    i_final(4)
    i_final(5)
    i_final(6)
    i_final(7)
    for at, n in cut(HID):
        v = mm(cht[at : at + n], c_all[...].reshape(1024, W)) * (p_h / TOP)
        dg[at : at + n] = (sum(mm(h64[:n, :n], p) for p in split(v, 2)) * R64).astype(bf16)
    weight_grad(gat, gg)
    weight_grad(uat, ug)
    scale = p_h * p_d / (TOP * TOP)
    net.wait(o_cross, oxr.at[pl.ds(1, NX - 1)])
    v = o_part[ZERO, x, :, 256:512]
    for j in range(1, NX):
        v = v + oxr[j].astype(f32)
    out[:, 256:512] = (v * scale).astype(bf16)
    net.wait(left_owner, lzr.at[pl.ds(3, 4)])
    v = o_part[ZERO, x, :, 0:256]
    for n in range(3, 7):
        v = v + lzr[n].astype(f32)
    out[:, 0:256] = (v * scale).astype(bf16)
    v = izf[0]
    net.count(izs.at[0], NZ - 1)
    net.wait(i_owner, izr.at[pl.ds(1, NZ - 1)])
    for d in range(1, NZ):
        v = v + izr[d].astype(f32)
    ig[...] = (turn_cols(v, h128, 3) * R128).astype(bf16)
    net.wait_sent(unread)


def hand_over(*refs):
    n = len(refs) // 2
    copies = [pltpu.make_async_copy(refs[i], refs[n + i], refs[-1].at[i]) for i in range(n)]
    for copy in copies:
        copy.start()
    for copy in copies:
        copy.wait()


def shards(tokens, cotangent, gate_weight, up_weight, down_weight):
    def vm(shape, dtype):
        return pltpu.VMEM(shape, dtype)

    part = (NZ, NX, ROWS, W)
    scratch = [
        vm((ROWS, W), bf16), vm((ROWS, W), bf16),
        vm((256, 256), bf16), vm((256, 256), bf16), vm((3, HID, W), bf16),
        vm(part, bf16), vm(part, bf16), vm((8, 128, W), bf16),
        vm((HID, W), f32), vm((HID, W), f32), vm((HID, W), f32),
        vm((HID, W), bf16), vm((HID, W), bf16), vm((HID, W), bf16),
        vm((3, 8, 128), f32), vm((17, 8, 128), f32), vm((3, 8, 128), f32), vm((17, 8, 128), f32),
        vm((8, 128), f32), vm((8, 128), f32),
        vm((4, 128, PAIR), f32), vm((4, 128, PAIR), f32), vm((4, 128, PAIR), f32),
        vm((6, 96, PAIR), bf16), vm((2, 96, PAIR), bf16), vm((2, 2, 96, PAIR), bf16),
        vm((4, 64, PAIR), f32), vm((4, 64, PAIR), f32), vm((4, 64, PAIR), f32),
        vm((6, 32, PAIR), bf16), vm((2, 32, PAIR), bf16), vm((2, 2, 32, PAIR), bf16),
        vm((NY, NC, 64, PAIR), bf16), vm((NY, NC, 128, PAIR), bf16), vm((8, 64, PAIR), f32),
        vm((HID, 1024), bf16), vm((HID, 1024), bf16), vm((HID, 1024), bf16),
        vm(part, f32), vm((2, 4, NX, ROWS, 256), bf16), vm((2, 4, NX, ROWS, 256), bf16),
        vm((NX, ROWS, 256), bf16), vm((NX, ROWS, 256), bf16),
        vm((4, 3, 2, ROWS, 256), bf16), vm((4, 2, ROWS, 256), bf16), vm((4, 2, 2, ROWS, 256), bf16),
        vm((8, ROWS, 256), bf16), vm((7, ROWS, 256), bf16),
        vm(part, f32), vm((8, 3, ROWS, W), bf16), vm((8, ROWS, W), bf16), vm((8, 2, ROWS, W), bf16),
        vm((NZ, ROWS, W), f32), vm((NZ, ROWS, W), bf16), vm((NZ, ROWS, W), bf16),
        vm((MOST_SENT, 8, 128), f32),
        pltpu.SemaphoreType.DMA((N_PHASES,)), pltpu.SemaphoreType.DMA((N_SEMS,)), pltpu.SemaphoreType.DMA((5,)),
    ]
    vmem = pl.BlockSpec(memory_space=pltpu.VMEM)
    hbm = pl.BlockSpec(memory_space=pltpu.HBM)
    shapes = [jax.ShapeDtypeStruct((HID, W), bf16)] * 3 + [jax.ShapeDtypeStruct((ROWS, W), bf16)] * 2
    args = (tokens, cotangent, gate_weight.T, up_weight.T, down_weight)
    results = pl.pallas_call(
        kernel,
        out_shape=shapes,
        in_specs=[hbm] * 5,
        out_specs=[vmem] * 5,
        scratch_shapes=scratch,
        compiler_params=pltpu.CompilerParams(
            collective_id=0, has_side_effects=True, vmem_limit_bytes=44 * 1024 * 1024
        ),
    )(*(pltpu.with_memory_space_constraint(a, pltpu.HBM) for a in args))
    gg, ug, dg, out, ig = pl.pallas_call(
        hand_over,
        out_shape=shapes,
        in_specs=[vmem] * 5,
        out_specs=[hbm] * 5,
        scratch_shapes=[pltpu.SemaphoreType.DMA((5,))],
        compiler_params=pltpu.CompilerParams(vmem_limit_bytes=4 * 1024 * 1024),
    )(*results)
    return out, ig, gg.T, ug.T, dg


def solution(mesh):
    fine = Mesh(mesh.devices.reshape(NY, NC, NZ, NX), GX + GY)
    specs = (P(GY, GX), P(GY, GX), P(GX, GY), P(GX, GY), P(GY, GX))
    return jax.shard_map(
        shards, mesh=fine, in_specs=specs, out_specs=specs, check_vma=False
    )
```

```python
import functools

import jax
import jax.numpy as jnp
from jax import lax
from jax.experimental import pallas as pl
from jax.experimental.pallas import tpu as pltpu
from jax.sharding import Mesh
from jax.sharding import PartitionSpec as P

GY = ("gy_0", "gy_1")
GX = ("gx_0", "gx_1")
NY, NC, NZ, NX = 4, 2, 8, 4
MESH = pl.DeviceIdType.MESH
f32 = jnp.float32
bf16 = jnp.bfloat16

TOP = 448.0
TINY = 1e-6
ROWS = 32
W = 512
HID = 448
PAIR = 2 * HID
R128 = 128 ** -0.5
R64 = 64 ** -0.5


def mm(a, b):
    return lax.dot_general(a, b, (((1,), (0,)), ((), ())), preferred_element_type=f32)


def mm_t(a, b):
    return lax.dot_general(a, b, (((1,), (1,)), ((), ())), preferred_element_type=f32)


def table(size, block):
    i = lax.broadcasted_iota(jnp.int32, (size, size), 0)
    j = lax.broadcasted_iota(jnp.int32, (size, size), 1)
    v = i & j & (block - 1)
    v = v ^ (v >> 4)
    v = v ^ (v >> 2)
    v = v ^ (v >> 1)
    sign = 1 - 2 * (v & 1)
    same = (i & ~(block - 1)) == (j & ~(block - 1))
    return jnp.where(same, sign, 0).astype(f32).astype(bf16)


def cut(n):
    at = 0
    while at < n:
        yield at, min(256, n - at)
        at += 256


def split(v, terms):
    parts = []
    for _ in range(terms):
        p = v.astype(bf16)
        parts.append(p)
        v = v - p.astype(f32)
    return parts


def turn_cols(v, h, terms=1):
    parts = split(v, terms) if terms > 1 else [v]
    outs = []
    for at, n in cut(v.shape[1]):
        outs.append(sum(mm(p[:, at : at + n], h[:n, :n]) for p in parts))
    return jnp.concatenate(outs, axis=1)


def encode(v, dst):
    hi = v.astype(bf16)
    dst[0:64] = hi
    hi = hi.astype(f32)
    unit = jnp.abs(hi) * (2.0**-8 / 7.0)
    n = jnp.where(unit > 0, (v - hi) / jnp.where(unit > 0, unit, 1.0), 0.0)
    n = jnp.clip(jnp.floor(n + 0.5), -7.0, 7.0) + 7.0
    dst[64:96] = (n[0:32] * 15.0 + n[32:64]).astype(bf16)


def decode(src):
    hi = src[0:64].astype(f32)
    code = src[64:96].astype(f32)
    first = jnp.floor((code + 0.5) * (1.0 / 15.0))
    n = jnp.concatenate([first, code - first * 15.0], axis=0) - 7.0
    return hi + n * (jnp.abs(hi) * (2.0**-8 / 7.0))


class Net:
    def __init__(self, send, recv):
        self.send_sems, self.recv_sems = send, recv
        self.n = self.phase = 0
        self.sent = [0] * N_PHASES

    def sem(self):
        self.n += 1
        return self.n - 1

    def copy(self, src, dst, sem, **dev):
        names = {"y": "gx_0", "c": "gx_1", "z": "gy_0", "x": "gy_1"}
        return pltpu.make_async_remote_copy(
            src_ref=src,
            dst_ref=dst,
            send_sem=self.send_sems.at[self.phase],
            recv_sem=self.recv_sems.at[sem],
            device_id={names[k]: v for k, v in dev.items()},
            device_id_type=MESH,
        )

    def count(self, src, copies=1):
        size = copies * src.dtype.itemsize
        for n in src.shape:
            size *= n
        self.sent[self.phase] += size

    def send(self, src, dst, sem=None, **dev):
        d = self.copy(src, dst, self.sem() if sem is None else sem, **dev)
        d.start()
        self.count(src)
        return d

    def wait(self, sem, ref):
        self.copy(ref, ref, sem, c=1 - lax.axis_index("gx_1")).wait_recv()

    def wait_sent(self, ref):
        for self.phase in range(N_PHASES):
            part = ref.at[pl.ds(0, self.sent[self.phase] // 4096)]
            self.copy(part, part, 0, c=1 - lax.axis_index("gx_1")).wait_send()


class Peaks:
    def __init__(self, net, src, buf, me):
        self.net, self.src, self.buf = net, src, buf
        self.y, self.c, self.z, self.x = me

    def start(self, v):
        self.src[0] = v
        self.sem = self.net.sem()
        for j in range(1, 8):
            dy, dc = j // 2, j % 2
            self.net.send(
                self.src.at[0], self.buf.at[j - 1], self.sem, y=(self.y + dy) % NY, c=(self.c + dc) % NC
            )

    def gathered(self, level, at, n):
        self.net.wait(self.sem, self.buf.at[pl.ds(at, n)])
        v = self.src[level]
        for j in range(n):
            v = jnp.maximum(v, self.buf[at + j])
        return v

    def second(self):
        self.src[1] = self.gathered(0, 0, 7)
        self.sem = self.net.sem()
        for j in range(1, NX):
            self.net.send(self.src.at[1], self.buf.at[6 + j], self.sem, x=(self.x + j) % NX)

    def third(self):
        self.src[2] = self.gathered(1, 7, 3)
        self.sem = self.net.sem()
        for j in range(1, NZ):
            self.net.send(self.src.at[2], self.buf.at[9 + j], self.sem, z=(self.z + j) % NZ)

    def result(self):
        return self.gathered(2, 10, 7)


class ZX:
    def __init__(self, net, own, buf, z, x, width):
        self.net, self.own, self.buf, self.z, self.x = net, own, buf, z, x
        self.cols = pl.ds(0, width)
        self.came, self.crossed = {}, {}
        self.far, self.relays = net.sem(), net.sem()

    def at(self, d):
        return (self.z + d + NZ) % NZ

    def start(self):
        for d in (1, -1, 2, -2):
            self.came[-d] = self.net.send(self.own, self.buf.at[self.z, self.x, :, self.cols], z=self.at(d))

    def forward(self, d):
        self.came[d].wait_recv()
        to = self.at(2 if d < 0 else -2)
        block = self.buf.at[self.at(d), self.x, :, self.cols]
        if abs(d) == 1:
            self.came[3 * d] = self.net.send(block, block, z=to)
        else:
            half = self.buf.at[self.at(d), self.x, pl.ds(0 if d < 0 else 16, 16), self.cols]
            self.net.send(half, half, self.far, z=to)

    def cross(self, d):
        b = self.at(d)
        src = self.buf.at[b, self.x, :, self.cols] if d else self.own
        if abs(d) == 3:
            self.came[d].wait_recv()
        if d == 4:
            self.net.wait(self.far, self.buf.at[0, 0, :, self.cols])
        self.crossed[d] = self.net.sem()
        for k in (1, 3):
            self.net.send(src, self.buf.at[b, self.x, :, self.cols], self.crossed[d], x=(self.x + k) % NX)

    def relay(self, d):
        b, xp, xm = self.at(d), (self.x + 1) % NX, (self.x + 3) % NX
        self.net.wait(self.crossed[d], self.buf.at[0, pl.ds(0, 2), :, self.cols])
        lo = self.buf.at[b, xm, pl.ds(0, 16), self.cols]
        self.net.send(lo, lo, self.relays, x=xp)
        hi = self.buf.at[b, xp, pl.ds(16, 16), self.cols]
        self.net.send(hi, hi, self.relays, x=xm)

    def done(self):
        self.net.wait(self.relays, self.buf.at[pl.ds(0, 2), :, :, self.cols])


class XZ:
    def __init__(self, net, own, buf, z, x):
        self.net, self.own, self.buf, self.z, self.x = net, own, buf, z, x
        self.came = {}
        self.near, self.far = net.sem(), net.sem()
        self.cols = pl.ds(W - 128, 128)

    def block(self, d, at=0, n=NX):
        return self.buf.at[(self.z + d + NZ) % NZ, pl.ds(at, n), :, self.cols]

    def start(self):
        for j in (1, 3, 2):
            dst = self.buf.at[self.z, self.x, :, self.cols]
            self.net.send(self.own, dst, self.near, x=(self.x + j) % NX)

    def second(self):
        self.net.wait(self.near, self.buf.at[0, pl.ds(0, NX - 1), :, self.cols])
        for d in (1, -1, 2, -2):
            self.came[-d] = self.net.send(self.block(0), self.block(0), z=(self.z + d + NZ) % NZ)

    def forward(self, d):
        self.came[d].wait_recv()
        to = (self.z + (2 if d < 0 else NZ - 2)) % NZ
        if abs(d) == 1:
            self.came[3 * d] = self.net.send(self.block(d), self.block(d), z=to)
        else:
            half = self.block(d, 0 if d < 0 else 2, 2)
            self.net.send(half, half, self.far, z=to)

    def done(self):
        self.came[3].wait_recv()
        self.came[-3].wait_recv()
        self.net.wait(self.far, self.block(0))


class Gather:
    def __init__(self, net, buf, half, y, c, together):
        self.net, self.buf, self.half, self.y, self.c = net, buf, half, y, c
        self.yp, self.ym, self.y2 = (y + 1) % NY, (y + 3) % NY, (y + 2) % NY
        self.pair = net.sem() if together else None
        self.rest = net.sem()

    def part(self, y, i):
        return self.buf.at[y, self.c, pl.ds(i * self.half, self.half)]

    def to_pair(self, y):
        return self.net.send(self.buf.at[y, self.c], self.buf.at[y, self.c], self.pair, c=1 - self.c)

    def start(self):
        send, y = self.net.send, self.y
        self.p0 = send(self.part(y, 0), self.part(y, 0), y=self.yp)
        self.m1 = send(self.part(y, 1), self.part(y, 1), y=self.ym)
        self.own = self.to_pair(y)

    def start_rest(self):
        send, y = self.net.send, self.y
        self.p1 = send(self.part(y, 1), self.part(y, 1), y=self.yp)
        self.m0 = send(self.part(y, 0), self.part(y, 0), y=self.ym)

    def relay(self):
        send = self.net.send
        self.p0.wait_recv()
        send(self.part(self.ym, 0), self.part(self.ym, 0), self.rest, y=self.yp)
        self.m1.wait_recv()
        send(self.part(self.yp, 1), self.part(self.yp, 1), self.rest, y=self.ym)

    def share(self):
        self.p1.wait_recv()
        self.fp = self.to_pair(self.ym)
        self.m0.wait_recv()
        self.fm = self.to_pair(self.yp)

    def last(self):
        self.net.wait(self.rest, self.buf.at[0, 0])
        self.f2 = self.to_pair(self.y2)

    def done(self):
        self.net.wait(self.pair, self.buf.at[:, 0])


N_SEMS = 126
N_PHASES = 5
MOST_SENT = 1280
RELATIVE = (3, -3, 4, 0, 2, -2, 1, -1)


def kernel(
    tok_hbm, cot_hbm, wg_hbm, wu_hbm, wd_hbm,
    gg, ug, dg, out, ig,
    tok, cot, h128, h64, wts, t_all, c_all, tc, rg, ru, rd, cg, cu, cd,
    pk_src, pk_buf, ph_src, ph_buf, pk, ph,
    dsrc, drecv, acc, ysrc, yrel, yfin, esrc, erecv, eacc, bsrc, brel, bfin,
    h_all, a_all, hrot, cht, gat, uat,
    o_part, osrc, orecv, oxs, oxr, lsrc, lrel, lfin, lzs, lzr,
    i_part, isrc, irel, ifin, izf, izs, izr,
    unread,
    ssem, rsem, lsem,
):
    y = lax.axis_index("gx_0")
    c = lax.axis_index("gx_1")
    z = lax.axis_index("gy_0")
    x = lax.axis_index("gy_1")
    pc = 1 - c
    net = Net(ssem, rsem)
    send = net.send
    yp, ym, y2 = (y + 1) % NY, (y + 3) % NY, (y + 2) % NY
    xp, xm, x2 = (x + 1) % NX, (x + 3) % NX, (x + 2) % NX
    zp, zm = (z + 1) % NZ, (z + 7) % NZ

    def zat(d):
        return (z + d + NZ) % NZ

    barrier = pltpu.get_barrier_semaphore()
    for j in range(1, 8):
        pl.semaphore_signal(
            barrier, inc=1, device_id={"gx_0": (y + j // 2) % NY, "gx_1": (c + j % 2) % NC},
            device_id_type=MESH,
        )
    for j in range(1, NX):
        pl.semaphore_signal(barrier, inc=1, device_id={"gy_1": (x + j) % NX}, device_id_type=MESH)
    for j in range(1, NZ):
        pl.semaphore_signal(barrier, inc=1, device_id={"gy_0": (z + j) % NZ}, device_id_type=MESH)
    loads = [
        pltpu.make_async_copy(src, dst, lsem.at[i])
        for i, (src, dst) in enumerate(
            (
                (tok_hbm, tok), (cot_hbm, cot),
                (wg_hbm, wts.at[0]), (wu_hbm, wts.at[1]), (wd_hbm, wts.at[2]),
            )
        )
    ]
    for load in loads:
        load.start()
    h128[...] = table(256, 128)
    h64[...] = table(256, 64)
    for load in loads:
        load.wait()
    t_all[z, x] = tok[...]
    c_all[z, x] = cot[...]

    def rotate_weights():
        rg[...] = turn_cols(wts[0], h128) * R128
        ru[...] = turn_cols(wts[1], h128) * R128
        for at, n in cut(HID):
            rd[at : at + n] = mm(h64[:n, :n], wts[2, at : at + n]) * R64

    p_x = jnp.max(jnp.abs(turn_cols(tok[...], h128))) * R128
    rotate_weights()
    p_g = jnp.max(jnp.abs(rg[...]))
    p_u = jnp.max(jnp.abs(ru[...]))
    p_d = jnp.max(jnp.abs(rd[...]))
    row = lax.broadcasted_iota(jnp.int32, (8, 128), 0)
    own_peaks = jnp.where(row == 0, p_x, jnp.where(row == 1, p_g, jnp.where(row == 2, p_u, p_d)))
    pl.semaphore_wait(barrier, 7 + 3 + 7)

    T = ZX(net, tok.at[:, pl.ds(0, W - 128)], t_all, z, x, W - 128)
    A = XZ(net, tok.at[:, pl.ds(W - 128, 128)], t_all, z, x)
    C = ZX(net, cot, c_all, z, x, W)
    peaks = Peaks(net, pk_src, pk_buf, (y, c, z, x))
    A.start()
    T.start()
    peaks.start(own_peaks)
    T.cross(0)
    T.forward(1)
    T.forward(-1)
    A.second()
    peaks.second()
    T.cross(1)
    T.cross(-1)
    for d in (2, -2):
        T.forward(d)
        T.cross(d)
    T.relay(0)
    for d in (1, -1):
        A.forward(d)
    T.relay(1)
    T.relay(-1)
    for d in (2, -2):
        A.forward(d)
    T.cross(3)
    T.cross(-3)
    T.cross(4)
    peaks.third()
    net.phase = 1
    C.start()
    T.relay(2)
    T.relay(-2)
    T.relay(3)
    T.relay(-3)
    T.relay(4)
    pk[...] = peaks.result()
    inv_x = 1.0 / (pk[0:1, 0:1] + TINY)
    cg[...] = (TOP * jnp.tanh(rg[...] * (1.0 / (pk[1:2, 0:1] + TINY)))).astype(bf16)
    cu[...] = (TOP * jnp.tanh(ru[...] * (1.0 / (pk[2:3, 0:1] + TINY)))).astype(bf16)
    A.done()
    T.done()
    for d in (1, -1, 2, -2):
        C.forward(d)
    for d in (0, 1, -1, 2, -2):
        C.cross(d)

    def gate_up(k, dst):
        t = turn_cols(t_all[k].reshape(4 * ROWS, W), h128)
        t = (TOP * jnp.tanh(t * (R128 * inv_x))).astype(bf16)
        tc[k] = t
        dst[:, 0:HID] = mm_t(t, cg[...])
        dst[:, HID:PAIR] = mm_t(t, cu[...])

    order = [y2, yp, ym, y]
    dh, eh = {}, {}

    def pair_part(i):
        gate_up(order[i] * 2 + pc, dsrc.at[i])
        if i == 0:
            first, last = pl.ds(0, 64), pl.ds(64, 64)
            dh["first"] = send(dsrc.at[0, first], drecv.at[0, first], c=pc)
            dh[0] = send(dsrc.at[0, last], drecv.at[0, last], c=pc)
        else:
            dh[i] = send(dsrc.at[i], drecv.at[i], c=pc)

    def own_part(i):
        gate_up(order[i] * 2 + c, acc.at[i])

    def q(i, at):
        return acc[i, at : at + 64] + drecv[i, at : at + 64]

    def put(slot, v, dst, sem=None, **dev):
        encode(v, ysrc.at[slot])
        return send(ysrc.at[slot], dst, sem, **dev)

    net.phase = 2
    y_fin, b_fin = net.sem(), net.sem()
    pair_part(0)
    pair_part(1)
    own_part(0)
    dh["first"].wait_recv()
    relp = put(0, q(0, 0), yrel.at[0], y=yp)
    dh[0].wait_recv()
    relm = put(1, q(0, 64), yrel.at[1], y=ym)
    own_part(1)
    C.cross(3)
    C.cross(-3)
    C.cross(4)
    pair_part(2)
    C.relay(0)
    C.relay(1)
    C.relay(-1)
    own_part(2)
    dh[1].wait_recv()
    put(2, q(1, 64), yfin.at[0, 1], y_fin, y=yp)
    dh[2].wait_recv()
    put(3, q(2, 0), yfin.at[1, 0], y_fin, y=ym)
    C.relay(2)
    C.relay(-2)
    cd[...] = (TOP * jnp.tanh(rd[...] * (1.0 / (pk[3:4, 0:1] + TINY)))).astype(bf16)
    pair_part(3)
    C.relay(3)
    C.relay(-3)
    C.relay(4)
    relp.wait_recv()
    put(4, q(1, 0) + decode(yrel.at[0]), yfin.at[0, 0], y_fin, y=yp)
    relm.wait_recv()
    put(5, q(2, 64) + decode(yrel.at[1]), yfin.at[1, 1], y_fin, y=ym)
    own_part(3)
    C.done()

    def back(k, dst):
        b = mm_t(c_all[k].reshape(4 * ROWS, W), cd[...])
        dst[:, 0:HID] = b[0:64]
        dst[:, HID:PAIR] = b[64:128]

    def e(i, at):
        return eacc[i, at : at + 32] + erecv[i, at : at + 32]

    def put_b(slot, v, dst, sem=None, **dev):
        bsrc[slot] = v.astype(bf16)
        return send(bsrc.at[slot], dst, sem, **dev)

    for i in range(4):
        back(order[i] * 2 + pc, esrc.at[i])
        eh[i] = send(esrc.at[i], erecv.at[i], c=pc)
    for i in range(4):
        back(order[i] * 2 + c, eacc.at[i])
        if i == 0:
            eh[0].wait_recv()
            brp = put_b(0, e(0, 0), brel.at[0], y=yp)
            brm = put_b(1, e(0, 32), brel.at[1], y=ym)
    eh[1].wait_recv()
    put_b(2, e(1, 32), bfin.at[0, 1], b_fin, y=yp)
    eh[2].wait_recv()
    put_b(3, e(2, 0), bfin.at[1, 0], b_fin, y=ym)

    p_x, p_g, p_u, p_d = (pk[i : i + 1, 0:1] for i in range(4))

    blocks = [(y, c), (y, pc), (ym, c), (yp, c), (ym, pc), (yp, pc), (y2, c), (y2, pc)]
    ir = {}
    i_fin = [net.sem() for _ in range(8)]
    i_owner = net.sem()

    def i_block(n):
        yy, cc = blocks[n]
        g = a_all[yy, cc, :, 0:HID]
        u = a_all[yy, cc, :, HID:PAIR]
        v = mm(g, cg[...]) * (p_g / TOP) + mm(u, cu[...]) * (p_u / TOP)
        i_part[n] = v.reshape(NX, ROWS, W)
        isrc[n, 0] = i_part[n, x2].astype(bf16)
        if n % 2 == 0:
            ir[n] = send(isrc.at[n, 0], irel.at[n], x=xp)
            isrc[n, 2] = i_part[n, xm].astype(bf16)
            send(isrc.at[n, 2], ifin.at[n, 1], i_fin[n], x=xm)
        else:
            ir[n] = send(isrc.at[n, 0], irel.at[n], x=xm)
            isrc[n, 1] = i_part[n, xp].astype(bf16)
            send(isrc.at[n, 1], ifin.at[n, 0], i_fin[n], x=xp)
        lanes = pl.ds(pl.multiple_of((yy * 2 + cc) * 128, 128), 128)
        gat[:, lanes] = g.T
        uat[:, lanes] = u.T

    def i_relay(n):
        ir[n].wait_recv()
        if n % 2 == 0:
            isrc[n, 1] = (i_part[n, xp] + irel[n].astype(f32)).astype(bf16)
            send(isrc.at[n, 1], ifin.at[n, 0], i_fin[n], x=xp)
        else:
            isrc[n, 2] = (i_part[n, xm] + irel[n].astype(f32)).astype(bf16)
            send(isrc.at[n, 2], ifin.at[n, 1], i_fin[n], x=xm)

    def i_final(n):
        yy, cc = blocks[n]
        net.wait(i_fin[n], ifin.at[n])
        k = yy * 2 + cc
        d = (k + NZ - z) % NZ
        v = i_part[n, x] + ifin[n, 0].astype(f32) + ifin[n, 1].astype(f32)
        izf[d] = v
        izs[d] = v.astype(bf16)

        @pl.when(d != 0)
        def _():
            net.copy(izs.at[d], izr.at[d], i_owner, z=k).start()

    dh[3].wait_recv()
    net.wait(y_fin, yfin)
    for i in range(2):
        acc[3, 64 * i : 64 * i + 64] = q(3, 64 * i) + decode(yfin.at[0, i]) + decode(yfin.at[1, i])
    gate = acc[3, :, 0:HID] * (p_x * p_g / (TOP * TOP))
    up = acc[3, :, HID:PAIR] * (p_x * p_u / (TOP * TOP))
    s = jax.nn.sigmoid(gate)
    hid = (gate * s * up).astype(bf16)
    h_all[y, c, :, 0:HID] = hid[0:64]
    h_all[y, c, :, HID:PAIR] = hid[64:128]
    hidp = Peaks(net, ph_src, ph_buf, (y, c, z, x))

    def turn_hidden(yy, cc):
        hrot[yy * 2 + cc] = turn_cols(h_all[yy, cc], h64) * R64

    turn_hidden(y, c)
    p_h = jnp.max(jnp.abs(hrot[y * 2 + c]))
    hidp.start(jnp.full((8, 128), p_h, f32))
    net.phase = 3
    H = Gather(net, h_all, 32, y, c, True)
    H.start()
    brp.wait_recv()
    put_b(4, e(1, 0) + brel[0].astype(f32), bfin.at[0, 0], b_fin, y=yp)
    brm.wait_recv()
    put_b(5, e(2, 32) + brel[1].astype(f32), bfin.at[1, 1], b_fin, y=ym)
    H.start_rest()
    hidp.second()
    H.relay()
    eh[3].wait_recv()
    net.wait(b_fin, bfin)
    b = jnp.concatenate(
        [e(3, 32 * i) + bfin[0, i].astype(f32) + bfin[1, i].astype(f32) for i in range(2)], axis=0
    )
    b = turn_cols(b * (p_d / TOP), h64, 3) * R64
    hg = jnp.concatenate([b[:, 0:HID], b[:, HID:PAIR]], axis=0)
    a_all[y, c, :, 0:HID] = (hg * up * s * (1.0 + gate * (1.0 - s))).astype(bf16)
    a_all[y, c, :, HID:PAIR] = (hg * gate * s).astype(bf16)
    G = Gather(net, a_all, 64, y, c, False)
    G.start()
    G.start_rest()
    net.phase = 4
    i_block(0)
    H.share()
    hidp.third()
    G.own.wait_recv()
    i_block(1)
    H.last()
    for yy in (ym, yp, y2):
        turn_hidden(yy, c)
    H.done()
    for yy in (y, ym, yp, y2):
        turn_hidden(yy, pc)
    G.relay()
    i_relay(0)
    i_relay(1)
    ph[...] = hidp.result()
    p_h = ph[0:1, 0:1]
    inv_h = 1.0 / (p_h + TINY)

    def o_block(d):
        k = zat(d)
        v = (TOP * jnp.tanh(hrot[k] * inv_h)).astype(bf16)
        v = jnp.concatenate([v[:, 0:HID], v[:, HID:PAIR]], axis=0)
        cht[:, pl.ds(pl.multiple_of(k * 128, 128), 128)] = v.T
        o_part[RELATIVE.index(d)] = mm(v, cd[...]).reshape(NX, ROWS, W)

    left_r = {}
    left_fin = [net.sem() for _ in range(4)]
    left_owner, left_mid = net.sem(), net.sem()
    ZERO = RELATIVE.index(0)

    def left_send(g, way, dst, sem=None):
        to = xp if way == 1 else xm
        return send(lsrc.at[g, 0 if sem is None else way], dst, sem, x=to)

    def left_start(g):
        way = 1 if g % 2 == 0 else 2
        for i in range(2):
            lsrc[g, 0, i] = o_part[2 * g + i, x2, :, 0:256].astype(bf16)
        left_r[g] = left_send(g, way, lrel.at[g])
        for i in range(2):
            lsrc[g, 3 - way, i] = o_part[2 * g + i, xp if way == 2 else xm, :, 0:256].astype(bf16)
        left_send(g, 3 - way, lfin.at[g, 2 - way], left_fin[g])

    def left_relay(g):
        way = 1 if g % 2 == 0 else 2
        left_r[g].wait_recv()
        for i in range(2):
            v = o_part[2 * g + i, xp if way == 1 else xm, :, 0:256] + lrel[g, i].astype(f32)
            lsrc[g, way, i] = v.astype(bf16)
        left_send(g, way, lfin.at[g, way - 1], left_fin[g])

    def left_final(g):
        net.wait(left_fin[g], lfin.at[g])
        if g == 2:
            net.wait(left_mid, lzr.at[pl.ds(0, 3)])
        for i in range(2):
            n, d = 2 * g + i, RELATIVE[2 * g + i]
            v = o_part[n, x, :, 0:256] + lfin[g, 0, i].astype(f32) + lfin[g, 1, i].astype(f32)
            if abs(d) == 2:
                v = v + lzr[0 if d > 0 else 1].astype(f32)
                half = lzr[2].astype(f32)
                rows = lax.broadcasted_iota(jnp.int32, (ROWS, 256), 0)
                v = v + jnp.where((rows < 16) if d > 0 else (rows >= 16), half, 0.0)
            if d == 0:
                o_part[n, x, :, 0:256] = v
                continue
            lzs[n] = v.astype(bf16)
            if d == 4:
                for at, to in ((0, 2), (16, -2)):
                    rows = pl.ds(at, 16)
                    send(lzs.at[n, rows], lzr.at[2, rows], left_mid, z=zat(to))
            elif abs(d) == 3:
                send(lzs.at[n], lzr.at[0 if d > 0 else 1], left_mid, z=zat(d // 3))
            else:
                send(lzs.at[n], lzr.at[3 + RELATIVE[4:].index(d)], left_owner, z=zat(d))

    op, om = {}, {}
    o_last, o_cross = net.sem(), net.sem()

    def o_ring(s):
        for side, d, handles, dev in ((0, 4 - s, op, zp), (1, s - 4, om, zm)):
            i = RELATIVE.index(4 if s == 0 else d)
            for j in (2, 3, 0, 1) if side == 0 else (0, 1, 2, 3):
                if s == 0 and (j < 2) != (side == 0):
                    continue
                v = o_part[i, j, :, 256:512]
                if (s - 1, j) in handles:
                    handles[s - 1, j].wait_recv()
                    v = v + orecv[side, s - 1, j].astype(f32)
                osrc[side, s, j] = v.astype(bf16)
                sem = o_last if s == 3 else None
                handles[s, j] = send(osrc.at[side, s, j], orecv.at[side, s, j], sem, z=dev)

    o_block(4)
    o_ring(0)
    o_block(3)
    o_block(-3)
    left_start(0)
    o_block(0)
    left_start(1)
    i_final(0)
    i_final(1)
    o_block(2)
    o_block(-2)
    o_ring(1)
    G.share()
    left_start(2)
    o_block(1)
    o_block(-1)
    left_start(3)
    left_relay(0)
    left_relay(1)
    i_block(2)
    i_block(3)
    G.last()
    G.fp.wait_recv()
    i_block(4)
    G.fm.wait_recv()
    i_block(5)
    o_ring(2)
    i_block(6)
    G.f2.wait_recv()
    i_block(7)
    left_final(0)
    left_final(1)
    i_relay(2)
    i_relay(3)
    left_relay(2)
    left_relay(3)
    o_ring(3)
    i_relay(4)
    i_relay(5)
    i_relay(6)
    i_relay(7)
    i_final(2)
    i_final(3)
    left_final(2)
    left_final(3)

    def weight_grad(acts, dst):
        for at, n in cut(HID):
            v = mm(acts[at : at + n], tc[...].reshape(1024, W)) * (p_x / TOP)
            dst[at : at + n] = (turn_cols(v, h128, 2) * R128).astype(bf16)

    net.wait(o_last, orecv.at[:, 3])
    for j in range(NX):
        v = o_part[ZERO, j, :, 256:512] + orecv[0, 3, j].astype(f32) + orecv[1, 3, j].astype(f32)
        o_part[ZERO, j, :, 256:512] = v
        oxs[j] = v.astype(bf16)
    for j in range(1, NX):
        send(oxs.at[(x + j) % NX], oxr.at[j], o_cross, x=(x + j) % NX)
    i_final(4)
    i_final(5)
    i_final(6)
    i_final(7)
    for at, n in cut(HID):
        v = mm(cht[at : at + n], c_all[...].reshape(1024, W)) * (p_h / TOP)
        dg[at : at + n] = (sum(mm(h64[:n, :n], p) for p in split(v, 2)) * R64).astype(bf16)
    weight_grad(gat, gg)
    weight_grad(uat, ug)
    scale = p_h * p_d / (TOP * TOP)
    net.wait(o_cross, oxr.at[pl.ds(1, NX - 1)])
    v = o_part[ZERO, x, :, 256:512]
    for j in range(1, NX):
        v = v + oxr[j].astype(f32)
    out[:, 256:512] = (v * scale).astype(bf16)
    net.wait(left_owner, lzr.at[pl.ds(3, 4)])
    v = o_part[ZERO, x, :, 0:256]
    for n in range(3, 7):
        v = v + lzr[n].astype(f32)
    out[:, 0:256] = (v * scale).astype(bf16)
    v = izf[0]
    net.count(izs.at[0], NZ - 1)
    net.wait(i_owner, izr.at[pl.ds(1, NZ - 1)])
    for d in range(1, NZ):
        v = v + izr[d].astype(f32)
    ig[...] = (turn_cols(v, h128, 3) * R128).astype(bf16)
    net.wait_sent(unread)


def hand_over(*refs):
    n = len(refs) // 2
    copies = [pltpu.make_async_copy(refs[i], refs[n + i], refs[-1].at[i]) for i in range(n)]
    for copy in copies:
        copy.start()
    for copy in copies:
        copy.wait()


def shards(tokens, cotangent, gate_weight, up_weight, down_weight):
    def vm(shape, dtype):
        return pltpu.VMEM(shape, dtype)

    part = (NZ, NX, ROWS, W)
    scratch = [
        vm((ROWS, W), bf16), vm((ROWS, W), bf16),
        vm((256, 256), bf16), vm((256, 256), bf16), vm((3, HID, W), bf16),
        vm(part, bf16), vm(part, bf16), vm((8, 128, W), bf16),
        vm((HID, W), f32), vm((HID, W), f32), vm((HID, W), f32),
        vm((HID, W), bf16), vm((HID, W), bf16), vm((HID, W), bf16),
        vm((3, 8, 128), f32), vm((17, 8, 128), f32), vm((3, 8, 128), f32), vm((17, 8, 128), f32),
        vm((8, 128), f32), vm((8, 128), f32),
        vm((4, 128, PAIR), f32), vm((4, 128, PAIR), f32), vm((4, 128, PAIR), f32),
        vm((6, 96, PAIR), bf16), vm((2, 96, PAIR), bf16), vm((2, 2, 96, PAIR), bf16),
        vm((4, 64, PAIR), f32), vm((4, 64, PAIR), f32), vm((4, 64, PAIR), f32),
        vm((6, 32, PAIR), bf16), vm((2, 32, PAIR), bf16), vm((2, 2, 32, PAIR), bf16),
        vm((NY, NC, 64, PAIR), bf16), vm((NY, NC, 128, PAIR), bf16), vm((8, 64, PAIR), f32),
        vm((HID, 1024), bf16), vm((HID, 1024), bf16), vm((HID, 1024), bf16),
        vm(part, f32), vm((2, 4, NX, ROWS, 256), bf16), vm((2, 4, NX, ROWS, 256), bf16),
        vm((NX, ROWS, 256), bf16), vm((NX, ROWS, 256), bf16),
        vm((4, 3, 2, ROWS, 256), bf16), vm((4, 2, ROWS, 256), bf16), vm((4, 2, 2, ROWS, 256), bf16),
        vm((8, ROWS, 256), bf16), vm((7, ROWS, 256), bf16),
        vm(part, f32), vm((8, 3, ROWS, W), bf16), vm((8, ROWS, W), bf16), vm((8, 2, ROWS, W), bf16),
        vm((NZ, ROWS, W), f32), vm((NZ, ROWS, W), bf16), vm((NZ, ROWS, W), bf16),
        vm((MOST_SENT, 8, 128), f32),
        pltpu.SemaphoreType.DMA((N_PHASES,)), pltpu.SemaphoreType.DMA((N_SEMS,)), pltpu.SemaphoreType.DMA((5,)),
    ]
    vmem = pl.BlockSpec(memory_space=pltpu.VMEM)
    hbm = pl.BlockSpec(memory_space=pltpu.HBM)
    shapes = [jax.ShapeDtypeStruct((HID, W), bf16)] * 3 + [jax.ShapeDtypeStruct((ROWS, W), bf16)] * 2
    args = (tokens, cotangent, gate_weight.T, up_weight.T, down_weight)
    results = pl.pallas_call(
        kernel,
        out_shape=shapes,
        in_specs=[hbm] * 5,
        out_specs=[vmem] * 5,
        scratch_shapes=scratch,
        compiler_params=pltpu.CompilerParams(
            collective_id=0, has_side_effects=True, vmem_limit_bytes=44 * 1024 * 1024
        ),
    )(*(pltpu.with_memory_space_constraint(a, pltpu.HBM) for a in args))
    gg, ug, dg, out, ig = pl.pallas_call(
        hand_over,
        out_shape=shapes,
        in_specs=[vmem] * 5,
        out_specs=[hbm] * 5,
        scratch_shapes=[pltpu.SemaphoreType.DMA((5,))],
        compiler_params=pltpu.CompilerParams(vmem_limit_bytes=4 * 1024 * 1024),
    )(*results)
    return out, ig, gg.T, ug.T, dg


def solution(mesh):
    fine = Mesh(mesh.devices.reshape(NY, NC, NZ, NX), GX + GY)
    specs = (P(GY, GX), P(GY, GX), P(GX, GY), P(GX, GY), P(GY, GX))
    return jax.shard_map(
        shards, mesh=fine, in_specs=specs, out_specs=specs, check_vma=False
    )
```

```python
import functools

import jax
import jax.numpy as jnp
from jax import lax
from jax.experimental import pallas as pl
from jax.experimental.pallas import tpu as pltpu
from jax.sharding import Mesh
from jax.sharding import PartitionSpec as P

GY = ("gy_0", "gy_1")
GX = ("gx_0", "gx_1")
NY, NC, NZ, NX = 4, 2, 8, 4
MESH = pl.DeviceIdType.MESH
f32 = jnp.float32
bf16 = jnp.bfloat16

TOP = 448.0
TINY = 1e-6
ROWS = 32
W = 512
HID = 448
PAIR = 2 * HID
R128 = 128 ** -0.5
R64 = 64 ** -0.5


def mm(a, b):
    return lax.dot_general(a, b, (((1,), (0,)), ((), ())), preferred_element_type=f32)


def mm_t(a, b):
    return lax.dot_general(a, b, (((1,), (1,)), ((), ())), preferred_element_type=f32)


def table(size, block):
    i = lax.broadcasted_iota(jnp.int32, (size, size), 0)
    j = lax.broadcasted_iota(jnp.int32, (size, size), 1)
    v = i & j & (block - 1)
    v = v ^ (v >> 4)
    v = v ^ (v >> 2)
    v = v ^ (v >> 1)
    sign = 1 - 2 * (v & 1)
    same = (i & ~(block - 1)) == (j & ~(block - 1))
    return jnp.where(same, sign, 0).astype(f32).astype(bf16)


def cut(n):
    at = 0
    while at < n:
        yield at, min(256, n - at)
        at += 256


def split(v, terms):
    parts = []
    for _ in range(terms):
        p = v.astype(bf16)
        parts.append(p)
        v = v - p.astype(f32)
    return parts


def turn_cols(v, h, terms=1):
    parts = split(v, terms) if terms > 1 else [v]
    outs = []
    for at, n in cut(v.shape[1]):
        outs.append(sum(mm(p[:, at : at + n], h[:n, :n]) for p in parts))
    return jnp.concatenate(outs, axis=1)


def encode(v, dst):
    hi = v.astype(bf16)
    dst[0:64] = hi
    hi = hi.astype(f32)
    unit = jnp.abs(hi) * (2.0**-8 / 7.0)
    n = jnp.where(unit > 0, (v - hi) / jnp.where(unit > 0, unit, 1.0), 0.0)
    n = jnp.clip(jnp.floor(n + 0.5), -7.0, 7.0) + 7.0
    dst[64:96] = (n[0:32] * 15.0 + n[32:64]).astype(bf16)


def decode(src):
    hi = src[0:64].astype(f32)
    code = src[64:96].astype(f32)
    first = jnp.floor((code + 0.5) * (1.0 / 15.0))
    n = jnp.concatenate([first, code - first * 15.0], axis=0) - 7.0
    return hi + n * (jnp.abs(hi) * (2.0**-8 / 7.0))


class Net:
    def __init__(self, send, recv):
        self.send_sems, self.recv_sems = send, recv
        self.n = self.phase = 0
        self.sent = [0] * N_PHASES

    def sem(self):
        self.n += 1
        return self.n - 1

    def copy(self, src, dst, sem, **dev):
        names = {"y": "gx_0", "c": "gx_1", "z": "gy_0", "x": "gy_1"}
        return pltpu.make_async_remote_copy(
            src_ref=src,
            dst_ref=dst,
            send_sem=self.send_sems.at[self.phase],
            recv_sem=self.recv_sems.at[sem],
            device_id={names[k]: v for k, v in dev.items()},
            device_id_type=MESH,
        )

    def count(self, src, copies=1):
        size = copies * src.dtype.itemsize
        for n in src.shape:
            size *= n
        self.sent[self.phase] += size

    def send(self, src, dst, sem=None, **dev):
        d = self.copy(src, dst, self.sem() if sem is None else sem, **dev)
        d.start()
        self.count(src)
        return d

    def wait(self, sem, ref):
        self.copy(ref, ref, sem, c=1 - lax.axis_index("gx_1")).wait_recv()

    def wait_sent(self, ref):
        for self.phase in range(N_PHASES):
            part = ref.at[pl.ds(0, self.sent[self.phase] // 4096)]
            self.copy(part, part, 0, c=1 - lax.axis_index("gx_1")).wait_send()


class Peaks:
    def __init__(self, net, src, buf, me):
        self.net, self.src, self.buf = net, src, buf
        self.y, self.c, self.z, self.x = me

    def start(self, v):
        self.src[0] = v
        self.sem = self.net.sem()
        for j in range(1, 8):
            dy, dc = j // 2, j % 2
            self.net.send(
                self.src.at[0], self.buf.at[j - 1], self.sem, y=(self.y + dy) % NY, c=(self.c + dc) % NC
            )

    def gathered(self, level, at, n):
        self.net.wait(self.sem, self.buf.at[pl.ds(at, n)])
        v = self.src[level]
        for j in range(n):
            v = jnp.maximum(v, self.buf[at + j])
        return v

    def second(self):
        self.src[1] = self.gathered(0, 0, 7)
        self.sem = self.net.sem()
        for j in range(1, NX):
            self.net.send(self.src.at[1], self.buf.at[6 + j], self.sem, x=(self.x + j) % NX)

    def third(self):
        self.src[2] = self.gathered(1, 7, 3)
        self.sem = self.net.sem()
        for j in range(1, NZ):
            self.net.send(self.src.at[2], self.buf.at[9 + j], self.sem, z=(self.z + j) % NZ)

    def result(self):
        return self.gathered(2, 10, 7)


class ZX:
    def __init__(self, net, own, buf, z, x, width):
        self.net, self.own, self.buf, self.z, self.x = net, own, buf, z, x
        self.cols = pl.ds(0, width)
        self.came, self.crossed = {}, {}
        self.far, self.relays = net.sem(), net.sem()

    def at(self, d):
        return (self.z + d + NZ) % NZ

    def start(self):
        for d in (1, -1, 2, -2):
            self.came[-d] = self.net.send(self.own, self.buf.at[self.z, self.x, :, self.cols], z=self.at(d))

    def forward(self, d):
        self.came[d].wait_recv()
        to = self.at(2 if d < 0 else -2)
        block = self.buf.at[self.at(d), self.x, :, self.cols]
        if abs(d) == 1:
            self.came[3 * d] = self.net.send(block, block, z=to)
        else:
            half = self.buf.at[self.at(d), self.x, pl.ds(0 if d < 0 else 16, 16), self.cols]
            self.net.send(half, half, self.far, z=to)

    def cross(self, d):
        b = self.at(d)
        src = self.buf.at[b, self.x, :, self.cols] if d else self.own
        if abs(d) == 3:
            self.came[d].wait_recv()
        if d == 4:
            self.net.wait(self.far, self.buf.at[0, 0, :, self.cols])
        self.crossed[d] = self.net.sem()
        for k in (1, 3):
            self.net.send(src, self.buf.at[b, self.x, :, self.cols], self.crossed[d], x=(self.x + k) % NX)

    def relay(self, d):
        b, xp, xm = self.at(d), (self.x + 1) % NX, (self.x + 3) % NX
        self.net.wait(self.crossed[d], self.buf.at[0, pl.ds(0, 2), :, self.cols])
        lo = self.buf.at[b, xm, pl.ds(0, 16), self.cols]
        self.net.send(lo, lo, self.relays, x=xp)
        hi = self.buf.at[b, xp, pl.ds(16, 16), self.cols]
        self.net.send(hi, hi, self.relays, x=xm)

    def done(self):
        self.net.wait(self.relays, self.buf.at[pl.ds(0, 2), :, :, self.cols])


class XZ:
    def __init__(self, net, own, buf, z, x):
        self.net, self.own, self.buf, self.z, self.x = net, own, buf, z, x
        self.came = {}
        self.near, self.far = net.sem(), net.sem()
        self.cols = pl.ds(W - 128, 128)

    def block(self, d, at=0, n=NX):
        return self.buf.at[(self.z + d + NZ) % NZ, pl.ds(at, n), :, self.cols]

    def start(self):
        for j in (1, 3, 2):
            dst = self.buf.at[self.z, self.x, :, self.cols]
            self.net.send(self.own, dst, self.near, x=(self.x + j) % NX)

    def second(self):
        self.net.wait(self.near, self.buf.at[0, pl.ds(0, NX - 1), :, self.cols])
        for d in (1, -1, 2, -2):
            self.came[-d] = self.net.send(self.block(0), self.block(0), z=(self.z + d + NZ) % NZ)

    def forward(self, d):
        self.came[d].wait_recv()
        to = (self.z + (2 if d < 0 else NZ - 2)) % NZ
        if abs(d) == 1:
            self.came[3 * d] = self.net.send(self.block(d), self.block(d), z=to)
        else:
            half = self.block(d, 0 if d < 0 else 2, 2)
            self.net.send(half, half, self.far, z=to)

    def done(self):
        self.came[3].wait_recv()
        self.came[-3].wait_recv()
        self.net.wait(self.far, self.block(0))


class Gather:
    def __init__(self, net, buf, half, y, c, together):
        self.net, self.buf, self.half, self.y, self.c = net, buf, half, y, c
        self.yp, self.ym, self.y2 = (y + 1) % NY, (y + 3) % NY, (y + 2) % NY
        self.pair = net.sem() if together else None
        self.rest = net.sem()

    def part(self, y, i):
        return self.buf.at[y, self.c, pl.ds(i * self.half, self.half)]

    def to_pair(self, y):
        return self.net.send(self.buf.at[y, self.c], self.buf.at[y, self.c], self.pair, c=1 - self.c)

    def start(self):
        send, y = self.net.send, self.y
        self.p0 = send(self.part(y, 0), self.part(y, 0), y=self.yp)
        self.m1 = send(self.part(y, 1), self.part(y, 1), y=self.ym)
        self.own = self.to_pair(y)

    def start_rest(self):
        send, y = self.net.send, self.y
        self.p1 = send(self.part(y, 1), self.part(y, 1), y=self.yp)
        self.m0 = send(self.part(y, 0), self.part(y, 0), y=self.ym)

    def relay(self):
        send = self.net.send
        self.p0.wait_recv()
        send(self.part(self.ym, 0), self.part(self.ym, 0), self.rest, y=self.yp)
        self.m1.wait_recv()
        send(self.part(self.yp, 1), self.part(self.yp, 1), self.rest, y=self.ym)

    def share(self):
        self.p1.wait_recv()
        self.fp = self.to_pair(self.ym)
        self.m0.wait_recv()
        self.fm = self.to_pair(self.yp)

    def last(self):
        self.net.wait(self.rest, self.buf.at[0, 0])
        self.f2 = self.to_pair(self.y2)

    def done(self):
        self.net.wait(self.pair, self.buf.at[:, 0])


N_SEMS = 126
N_PHASES = 5
MOST_SENT = 1280
RELATIVE = (3, -3, 4, 0, 2, -2, 1, -1)


def kernel(
    tok_hbm, cot_hbm, wg_hbm, wu_hbm, wd_hbm,
    gg, ug, dg, out, ig,
    tok, cot, h128, h64, wts, t_all, c_all, tc, rg, ru, rd, cg, cu, cd,
    pk_src, pk_buf, ph_src, ph_buf, pk, ph,
    dsrc, drecv, acc, ysrc, yrel, yfin, esrc, erecv, eacc, bsrc, brel, bfin,
    h_all, a_all, hrot, cht, gat, uat,
    o_part, osrc, orecv, oxs, oxr, lsrc, lrel, lfin, lzs, lzr,
    i_part, isrc, irel, ifin, izf, izs, izr,
    unread,
    ssem, rsem, lsem,
):
    y = lax.axis_index("gx_0")
    c = lax.axis_index("gx_1")
    z = lax.axis_index("gy_0")
    x = lax.axis_index("gy_1")
    pc = 1 - c
    net = Net(ssem, rsem)
    send = net.send
    yp, ym, y2 = (y + 1) % NY, (y + 3) % NY, (y + 2) % NY
    xp, xm, x2 = (x + 1) % NX, (x + 3) % NX, (x + 2) % NX
    zp, zm = (z + 1) % NZ, (z + 7) % NZ

    def zat(d):
        return (z + d + NZ) % NZ

    barrier = pltpu.get_barrier_semaphore()
    for j in range(1, 8):
        pl.semaphore_signal(
            barrier, inc=1, device_id={"gx_0": (y + j // 2) % NY, "gx_1": (c + j % 2) % NC},
            device_id_type=MESH,
        )
    for j in range(1, NX):
        pl.semaphore_signal(barrier, inc=1, device_id={"gy_1": (x + j) % NX}, device_id_type=MESH)
    for j in range(1, NZ):
        pl.semaphore_signal(barrier, inc=1, device_id={"gy_0": (z + j) % NZ}, device_id_type=MESH)
    loads = [
        pltpu.make_async_copy(src, dst, lsem.at[i])
        for i, (src, dst) in enumerate(
            (
                (tok_hbm, tok), (cot_hbm, cot),
                (wg_hbm, wts.at[0]), (wu_hbm, wts.at[1]), (wd_hbm, wts.at[2]),
            )
        )
    ]
    for load in loads:
        load.start()
    h128[...] = table(256, 128)
    h64[...] = table(256, 64)
    for load in loads:
        load.wait()
    t_all[z, x] = tok[...]
    c_all[z, x] = cot[...]

    def rotate_weights():
        rg[...] = turn_cols(wts[0], h128) * R128
        ru[...] = turn_cols(wts[1], h128) * R128
        for at, n in cut(HID):
            rd[at : at + n] = mm(h64[:n, :n], wts[2, at : at + n]) * R64

    p_x = jnp.max(jnp.abs(turn_cols(tok[...], h128))) * R128
    rotate_weights()
    p_g = jnp.max(jnp.abs(rg[...]))
    p_u = jnp.max(jnp.abs(ru[...]))
    p_d = jnp.max(jnp.abs(rd[...]))
    row = lax.broadcasted_iota(jnp.int32, (8, 128), 0)
    own_peaks = jnp.where(row == 0, p_x, jnp.where(row == 1, p_g, jnp.where(row == 2, p_u, p_d)))
    pl.semaphore_wait(barrier, 7 + 3 + 7)

    T = ZX(net, tok.at[:, pl.ds(0, W - 128)], t_all, z, x, W - 128)
    A = XZ(net, tok.at[:, pl.ds(W - 128, 128)], t_all, z, x)
    C = ZX(net, cot, c_all, z, x, W)
    peaks = Peaks(net, pk_src, pk_buf, (y, c, z, x))
    A.start()
    T.start()
    peaks.start(own_peaks)
    T.cross(0)
    T.forward(1)
    T.forward(-1)
    A.second()
    peaks.second()
    T.cross(1)
    T.cross(-1)
    for d in (2, -2):
        T.forward(d)
        T.cross(d)
    T.relay(0)
    for d in (1, -1):
        A.forward(d)
    T.relay(1)
    T.relay(-1)
    for d in (2, -2):
        A.forward(d)
    T.cross(3)
    T.cross(-3)
    T.cross(4)
    peaks.third()
    net.phase = 1
    C.start()
    T.relay(2)
    T.relay(-2)
    T.relay(3)
    T.relay(-3)
    T.relay(4)
    pk[...] = peaks.result()
    inv_x = 1.0 / (pk[0:1, 0:1] + TINY)
    cg[...] = (TOP * jnp.tanh(rg[...] * (1.0 / (pk[1:2, 0:1] + TINY)))).astype(bf16)
    cu[...] = (TOP * jnp.tanh(ru[...] * (1.0 / (pk[2:3, 0:1] + TINY)))).astype(bf16)
    for d in (1, -1, 2, -2):
        C.forward(d)
    A.done()
    T.done()
    for d in (0, 1, -1, 2, -2):
        C.cross(d)

    def gate_up(k, dst):
        t = turn_cols(t_all[k].reshape(4 * ROWS, W), h128)
        t = (TOP * jnp.tanh(t * (R128 * inv_x))).astype(bf16)
        tc[k] = t
        dst[:, 0:HID] = mm_t(t, cg[...])
        dst[:, HID:PAIR] = mm_t(t, cu[...])

    order = [y2, yp, ym, y]
    dh, eh = {}, {}

    def pair_part(i):
        gate_up(order[i] * 2 + pc, dsrc.at[i])
        if i == 0:
            first, last = pl.ds(0, 64), pl.ds(64, 64)
            dh["first"] = send(dsrc.at[0, first], drecv.at[0, first], c=pc)
            dh[0] = send(dsrc.at[0, last], drecv.at[0, last], c=pc)
        else:
            dh[i] = send(dsrc.at[i], drecv.at[i], c=pc)

    def own_part(i):
        gate_up(order[i] * 2 + c, acc.at[i])

    def q(i, at):
        return acc[i, at : at + 64] + drecv[i, at : at + 64]

    def put(slot, v, dst, sem=None, **dev):
        encode(v, ysrc.at[slot])
        return send(ysrc.at[slot], dst, sem, **dev)

    net.phase = 2
    y_fin, b_fin = net.sem(), net.sem()
    pair_part(0)
    pair_part(1)
    own_part(0)
    dh["first"].wait_recv()
    relp = put(0, q(0, 0), yrel.at[0], y=yp)
    dh[0].wait_recv()
    relm = put(1, q(0, 64), yrel.at[1], y=ym)
    own_part(1)
    C.cross(3)
    C.cross(-3)
    C.cross(4)
    pair_part(2)
    C.relay(0)
    C.relay(1)
    C.relay(-1)
    own_part(2)
    dh[1].wait_recv()
    put(2, q(1, 64), yfin.at[0, 1], y_fin, y=yp)
    dh[2].wait_recv()
    put(3, q(2, 0), yfin.at[1, 0], y_fin, y=ym)
    C.relay(2)
    C.relay(-2)
    cd[...] = (TOP * jnp.tanh(rd[...] * (1.0 / (pk[3:4, 0:1] + TINY)))).astype(bf16)
    pair_part(3)
    C.relay(3)
    C.relay(-3)
    C.relay(4)
    relp.wait_recv()
    put(4, q(1, 0) + decode(yrel.at[0]), yfin.at[0, 0], y_fin, y=yp)
    relm.wait_recv()
    put(5, q(2, 64) + decode(yrel.at[1]), yfin.at[1, 1], y_fin, y=ym)
    own_part(3)
    C.done()

    def back(k, dst):
        b = mm_t(c_all[k].reshape(4 * ROWS, W), cd[...])
        dst[:, 0:HID] = b[0:64]
        dst[:, HID:PAIR] = b[64:128]

    def e(i, at):
        return eacc[i, at : at + 32] + erecv[i, at : at + 32]

    def put_b(slot, v, dst, sem=None, **dev):
        bsrc[slot] = v.astype(bf16)
        return send(bsrc.at[slot], dst, sem, **dev)

    for i in range(4):
        back(order[i] * 2 + pc, esrc.at[i])
        eh[i] = send(esrc.at[i], erecv.at[i], c=pc)
    for i in range(4):
        back(order[i] * 2 + c, eacc.at[i])
        if i == 0:
            eh[0].wait_recv()
            brp = put_b(0, e(0, 0), brel.at[0], y=yp)
            brm = put_b(1, e(0, 32), brel.at[1], y=ym)
    eh[1].wait_recv()
    put_b(2, e(1, 32), bfin.at[0, 1], b_fin, y=yp)
    eh[2].wait_recv()
    put_b(3, e(2, 0), bfin.at[1, 0], b_fin, y=ym)

    p_x, p_g, p_u, p_d = (pk[i : i + 1, 0:1] for i in range(4))

    blocks = [(y, c), (y, pc), (ym, c), (yp, c), (ym, pc), (yp, pc), (y2, c), (y2, pc)]
    ir = {}
    i_fin = [net.sem() for _ in range(8)]
    i_owner = net.sem()

    def i_block(n):
        yy, cc = blocks[n]
        g = a_all[yy, cc, :, 0:HID]
        u = a_all[yy, cc, :, HID:PAIR]
        v = mm(g, cg[...]) * (p_g / TOP) + mm(u, cu[...]) * (p_u / TOP)
        i_part[n] = v.reshape(NX, ROWS, W)
        isrc[n, 0] = i_part[n, x2].astype(bf16)
        if n % 2 == 0:
            ir[n] = send(isrc.at[n, 0], irel.at[n], x=xp)
            isrc[n, 2] = i_part[n, xm].astype(bf16)
            send(isrc.at[n, 2], ifin.at[n, 1], i_fin[n], x=xm)
        else:
            ir[n] = send(isrc.at[n, 0], irel.at[n], x=xm)
            isrc[n, 1] = i_part[n, xp].astype(bf16)
            send(isrc.at[n, 1], ifin.at[n, 0], i_fin[n], x=xp)
        lanes = pl.ds(pl.multiple_of((yy * 2 + cc) * 128, 128), 128)
        gat[:, lanes] = g.T
        uat[:, lanes] = u.T

    def i_relay(n):
        ir[n].wait_recv()
        if n % 2 == 0:
            isrc[n, 1] = (i_part[n, xp] + irel[n].astype(f32)).astype(bf16)
            send(isrc.at[n, 1], ifin.at[n, 0], i_fin[n], x=xp)
        else:
            isrc[n, 2] = (i_part[n, xm] + irel[n].astype(f32)).astype(bf16)
            send(isrc.at[n, 2], ifin.at[n, 1], i_fin[n], x=xm)

    def i_final(n):
        yy, cc = blocks[n]
        net.wait(i_fin[n], ifin.at[n])
        k = yy * 2 + cc
        d = (k + NZ - z) % NZ
        v = i_part[n, x] + ifin[n, 0].astype(f32) + ifin[n, 1].astype(f32)
        izf[d] = v
        izs[d] = v.astype(bf16)

        @pl.when(d != 0)
        def _():
            net.copy(izs.at[d], izr.at[d], i_owner, z=k).start()

    dh[3].wait_recv()
    net.wait(y_fin, yfin)
    for i in range(2):
        acc[3, 64 * i : 64 * i + 64] = q(3, 64 * i) + decode(yfin.at[0, i]) + decode(yfin.at[1, i])
    gate = acc[3, :, 0:HID] * (p_x * p_g / (TOP * TOP))
    up = acc[3, :, HID:PAIR] * (p_x * p_u / (TOP * TOP))
    s = jax.nn.sigmoid(gate)
    hid = (gate * s * up).astype(bf16)
    h_all[y, c, :, 0:HID] = hid[0:64]
    h_all[y, c, :, HID:PAIR] = hid[64:128]
    hidp = Peaks(net, ph_src, ph_buf, (y, c, z, x))

    def turn_hidden(yy, cc):
        hrot[yy * 2 + cc] = turn_cols(h_all[yy, cc], h64) * R64

    turn_hidden(y, c)
    p_h = jnp.max(jnp.abs(hrot[y * 2 + c]))
    hidp.start(jnp.full((8, 128), p_h, f32))
    net.phase = 3
    H = Gather(net, h_all, 32, y, c, True)
    H.start()
    brp.wait_recv()
    put_b(4, e(1, 0) + brel[0].astype(f32), bfin.at[0, 0], b_fin, y=yp)
    brm.wait_recv()
    put_b(5, e(2, 32) + brel[1].astype(f32), bfin.at[1, 1], b_fin, y=ym)
    H.start_rest()
    hidp.second()
    H.relay()
    eh[3].wait_recv()
    net.wait(b_fin, bfin)
    b = jnp.concatenate(
        [e(3, 32 * i) + bfin[0, i].astype(f32) + bfin[1, i].astype(f32) for i in range(2)], axis=0
    )
    b = turn_cols(b * (p_d / TOP), h64, 3) * R64
    hg = jnp.concatenate([b[:, 0:HID], b[:, HID:PAIR]], axis=0)
    a_all[y, c, :, 0:HID] = (hg * up * s * (1.0 + gate * (1.0 - s))).astype(bf16)
    a_all[y, c, :, HID:PAIR] = (hg * gate * s).astype(bf16)
    G = Gather(net, a_all, 64, y, c, False)
    G.start()
    G.start_rest()
    net.phase = 4
    i_block(0)
    H.share()
    hidp.third()
    G.own.wait_recv()
    i_block(1)
    H.last()
    for yy in (ym, yp, y2):
        turn_hidden(yy, c)
    H.done()
    for yy in (y, ym, yp, y2):
        turn_hidden(yy, pc)
    G.relay()
    i_relay(0)
    i_relay(1)
    ph[...] = hidp.result()
    p_h = ph[0:1, 0:1]
    inv_h = 1.0 / (p_h + TINY)

    def o_block(d):
        k = zat(d)
        v = (TOP * jnp.tanh(hrot[k] * inv_h)).astype(bf16)
        v = jnp.concatenate([v[:, 0:HID], v[:, HID:PAIR]], axis=0)
        cht[:, pl.ds(pl.multiple_of(k * 128, 128), 128)] = v.T
        o_part[RELATIVE.index(d)] = mm(v, cd[...]).reshape(NX, ROWS, W)

    left_r = {}
    left_fin = [net.sem() for _ in range(4)]
    left_owner, left_mid = net.sem(), net.sem()
    ZERO = RELATIVE.index(0)

    def left_send(g, way, dst, sem=None):
        to = xp if way == 1 else xm
        return send(lsrc.at[g, 0 if sem is None else way], dst, sem, x=to)

    def left_start(g):
        way = 1 if g % 2 == 0 else 2
        for i in range(2):
            lsrc[g, 0, i] = o_part[2 * g + i, x2, :, 0:256].astype(bf16)
        left_r[g] = left_send(g, way, lrel.at[g])
        for i in range(2):
            lsrc[g, 3 - way, i] = o_part[2 * g + i, xp if way == 2 else xm, :, 0:256].astype(bf16)
        left_send(g, 3 - way, lfin.at[g, 2 - way], left_fin[g])

    def left_relay(g):
        way = 1 if g % 2 == 0 else 2
        left_r[g].wait_recv()
        for i in range(2):
            v = o_part[2 * g + i, xp if way == 1 else xm, :, 0:256] + lrel[g, i].astype(f32)
            lsrc[g, way, i] = v.astype(bf16)
        left_send(g, way, lfin.at[g, way - 1], left_fin[g])

    def left_final(g):
        net.wait(left_fin[g], lfin.at[g])
        if g == 2:
            net.wait(left_mid, lzr.at[pl.ds(0, 3)])
        for i in range(2):
            n, d = 2 * g + i, RELATIVE[2 * g + i]
            v = o_part[n, x, :, 0:256] + lfin[g, 0, i].astype(f32) + lfin[g, 1, i].astype(f32)
            if abs(d) == 2:
                v = v + lzr[0 if d > 0 else 1].astype(f32)
                half = lzr[2].astype(f32)
                rows = lax.broadcasted_iota(jnp.int32, (ROWS, 256), 0)
                v = v + jnp.where((rows < 16) if d > 0 else (rows >= 16), half, 0.0)
            if d == 0:
                o_part[n, x, :, 0:256] = v
                continue
            lzs[n] = v.astype(bf16)
            if d == 4:
                for at, to in ((0, 2), (16, -2)):
                    rows = pl.ds(at, 16)
                    send(lzs.at[n, rows], lzr.at[2, rows], left_mid, z=zat(to))
            elif abs(d) == 3:
                send(lzs.at[n], lzr.at[0 if d > 0 else 1], left_mid, z=zat(d // 3))
            else:
                send(lzs.at[n], lzr.at[3 + RELATIVE[4:].index(d)], left_owner, z=zat(d))

    op, om = {}, {}
    o_last, o_cross = net.sem(), net.sem()

    def o_ring(s):
        for side, d, handles, dev in ((0, 4 - s, op, zp), (1, s - 4, om, zm)):
            i = RELATIVE.index(4 if s == 0 else d)
            for j in (2, 3, 0, 1) if side == 0 else (0, 1, 2, 3):
                if s == 0 and (j < 2) != (side == 0):
                    continue
                v = o_part[i, j, :, 256:512]
                if (s - 1, j) in handles:
                    handles[s - 1, j].wait_recv()
                    v = v + orecv[side, s - 1, j].astype(f32)
                osrc[side, s, j] = v.astype(bf16)
                sem = o_last if s == 3 else None
                handles[s, j] = send(osrc.at[side, s, j], orecv.at[side, s, j], sem, z=dev)

    o_block(4)
    o_ring(0)
    o_block(3)
    o_block(-3)
    left_start(0)
    o_block(0)
    left_start(1)
    i_final(0)
    i_final(1)
    o_block(2)
    o_block(-2)
    o_ring(1)
    G.share()
    left_start(2)
    o_block(1)
    o_block(-1)
    left_start(3)
    left_relay(0)
    left_relay(1)
    i_block(2)
    i_block(3)
    G.last()
    G.fp.wait_recv()
    i_block(4)
    G.fm.wait_recv()
    i_block(5)
    o_ring(2)
    i_block(6)
    G.f2.wait_recv()
    i_block(7)
    left_final(0)
    left_final(1)
    i_relay(2)
    i_relay(3)
    left_relay(2)
    left_relay(3)
    o_ring(3)
    i_relay(4)
    i_relay(5)
    i_relay(6)
    i_relay(7)
    i_final(2)
    i_final(3)
    left_final(2)
    left_final(3)

    def weight_grad(acts, dst):
        for at, n in cut(HID):
            v = mm(acts[at : at + n], tc[...].reshape(1024, W)) * (p_x / TOP)
            dst[at : at + n] = (turn_cols(v, h128, 2) * R128).astype(bf16)

    net.wait(o_last, orecv.at[:, 3])
    for j in range(NX):
        v = o_part[ZERO, j, :, 256:512] + orecv[0, 3, j].astype(f32) + orecv[1, 3, j].astype(f32)
        o_part[ZERO, j, :, 256:512] = v
        oxs[j] = v.astype(bf16)
    for j in range(1, NX):
        send(oxs.at[(x + j) % NX], oxr.at[j], o_cross, x=(x + j) % NX)
    i_final(4)
    i_final(5)
    i_final(6)
    i_final(7)
    for at, n in cut(HID):
        v = mm(cht[at : at + n], c_all[...].reshape(1024, W)) * (p_h / TOP)
        dg[at : at + n] = (sum(mm(h64[:n, :n], p) for p in split(v, 2)) * R64).astype(bf16)
    weight_grad(gat, gg)
    weight_grad(uat, ug)
    scale = p_h * p_d / (TOP * TOP)
    net.wait(o_cross, oxr.at[pl.ds(1, NX - 1)])
    v = o_part[ZERO, x, :, 256:512]
    for j in range(1, NX):
        v = v + oxr[j].astype(f32)
    out[:, 256:512] = (v * scale).astype(bf16)
    net.wait(left_owner, lzr.at[pl.ds(3, 4)])
    v = o_part[ZERO, x, :, 0:256]
    for n in range(3, 7):
        v = v + lzr[n].astype(f32)
    out[:, 0:256] = (v * scale).astype(bf16)
    v = izf[0]
    net.count(izs.at[0], NZ - 1)
    net.wait(i_owner, izr.at[pl.ds(1, NZ - 1)])
    for d in range(1, NZ):
        v = v + izr[d].astype(f32)
    ig[...] = (turn_cols(v, h128, 3) * R128).astype(bf16)
    net.wait_sent(unread)


def hand_over(*refs):
    n = len(refs) // 2
    copies = [pltpu.make_async_copy(refs[i], refs[n + i], refs[-1].at[i]) for i in range(n)]
    for copy in copies:
        copy.start()
    for copy in copies:
        copy.wait()


def shards(tokens, cotangent, gate_weight, up_weight, down_weight):
    def vm(shape, dtype):
        return pltpu.VMEM(shape, dtype)

    part = (NZ, NX, ROWS, W)
    scratch = [
        vm((ROWS, W), bf16), vm((ROWS, W), bf16),
        vm((256, 256), bf16), vm((256, 256), bf16), vm((3, HID, W), bf16),
        vm(part, bf16), vm(part, bf16), vm((8, 128, W), bf16),
        vm((HID, W), f32), vm((HID, W), f32), vm((HID, W), f32),
        vm((HID, W), bf16), vm((HID, W), bf16), vm((HID, W), bf16),
        vm((3, 8, 128), f32), vm((17, 8, 128), f32), vm((3, 8, 128), f32), vm((17, 8, 128), f32),
        vm((8, 128), f32), vm((8, 128), f32),
        vm((4, 128, PAIR), f32), vm((4, 128, PAIR), f32), vm((4, 128, PAIR), f32),
        vm((6, 96, PAIR), bf16), vm((2, 96, PAIR), bf16), vm((2, 2, 96, PAIR), bf16),
        vm((4, 64, PAIR), f32), vm((4, 64, PAIR), f32), vm((4, 64, PAIR), f32),
        vm((6, 32, PAIR), bf16), vm((2, 32, PAIR), bf16), vm((2, 2, 32, PAIR), bf16),
        vm((NY, NC, 64, PAIR), bf16), vm((NY, NC, 128, PAIR), bf16), vm((8, 64, PAIR), f32),
        vm((HID, 1024), bf16), vm((HID, 1024), bf16), vm((HID, 1024), bf16),
        vm(part, f32), vm((2, 4, NX, ROWS, 256), bf16), vm((2, 4, NX, ROWS, 256), bf16),
        vm((NX, ROWS, 256), bf16), vm((NX, ROWS, 256), bf16),
        vm((4, 3, 2, ROWS, 256), bf16), vm((4, 2, ROWS, 256), bf16), vm((4, 2, 2, ROWS, 256), bf16),
        vm((8, ROWS, 256), bf16), vm((7, ROWS, 256), bf16),
        vm(part, f32), vm((8, 3, ROWS, W), bf16), vm((8, ROWS, W), bf16), vm((8, 2, ROWS, W), bf16),
        vm((NZ, ROWS, W), f32), vm((NZ, ROWS, W), bf16), vm((NZ, ROWS, W), bf16),
        vm((MOST_SENT, 8, 128), f32),
        pltpu.SemaphoreType.DMA((N_PHASES,)), pltpu.SemaphoreType.DMA((N_SEMS,)), pltpu.SemaphoreType.DMA((5,)),
    ]
    vmem = pl.BlockSpec(memory_space=pltpu.VMEM)
    hbm = pl.BlockSpec(memory_space=pltpu.HBM)
    shapes = [jax.ShapeDtypeStruct((HID, W), bf16)] * 3 + [jax.ShapeDtypeStruct((ROWS, W), bf16)] * 2
    args = (tokens, cotangent, gate_weight.T, up_weight.T, down_weight)
    results = pl.pallas_call(
        kernel,
        out_shape=shapes,
        in_specs=[hbm] * 5,
        out_specs=[vmem] * 5,
        scratch_shapes=scratch,
        compiler_params=pltpu.CompilerParams(
            collective_id=0, has_side_effects=True, vmem_limit_bytes=44 * 1024 * 1024
        ),
    )(*(pltpu.with_memory_space_constraint(a, pltpu.HBM) for a in args))
    gg, ug, dg, out, ig = pl.pallas_call(
        hand_over,
        out_shape=shapes,
        in_specs=[vmem] * 5,
        out_specs=[hbm] * 5,
        scratch_shapes=[pltpu.SemaphoreType.DMA((5,))],
        compiler_params=pltpu.CompilerParams(vmem_limit_bytes=4 * 1024 * 1024),
    )(*results)
    return out, ig, gg.T, ug.T, dg


def solution(mesh):
    fine = Mesh(mesh.devices.reshape(NY, NC, NZ, NX), GX + GY)
    specs = (P(GY, GX), P(GY, GX), P(GX, GY), P(GX, GY), P(GY, GX))
    return jax.shard_map(
        shards, mesh=fine, in_specs=specs, out_specs=specs, check_vma=False
    )
```
